32 devices in a mesh: dp: 1 (over z), dm: 4 (over y), tp: 8 (over x, core).
Axes of the slice: x: 4, y: 4, z: 1, core: 2. Of those that a mesh axis runs over, the one named last changes fastest.
The devices are a block of a 4x4x8 slice.
Arguments:
- hidden: bfloat16 [128, 4096], P('dp', 'dm')
- w_q: bfloat16 [4096, 32, 128], P('dm', 'tp')
- w_k: bfloat16 [4096, 32, 128], P('dm', 'tp')
- w_v: bfloat16 [4096, 32, 128], P('dm', 'tp')
- w_o: bfloat16 [32, 128, 4096], P('tp', None, 'dm')
- w_gate: bfloat16 [4096, 11008], P('dm', 'tp')
- w_up: bfloat16 [4096, 11008], P('dm', 'tp')
- w_down: bfloat16 [11008, 4096], P('tp', 'dm')
- norm_attn: bfloat16 [4096], P('dm')
- norm_mlp: bfloat16 [4096], P('dm')
- k_cache: bfloat16 [128, 256, 32, 128], P(('dp', 'dm'), None, 'tp')
- v_cache: bfloat16 [128, 256, 32, 128], P(('dp', 'dm'), None, 'tp')
- seq_lens: int32 [128], P(('dp', 'dm'))
- rope_cos: float32 [128, 64], P(('dp', 'dm'))
- rope_sin: float32 [128, 64], P(('dp', 'dm'))
Outputs:
- output 1: bfloat16 [128, 4096], P('dp', 'dm')
- output 2: bfloat16 [128, 256, 32, 128], P(('dp', 'dm'), None, 'tp')
- output 3: bfloat16 [128, 256, 32, 128], P(('dp', 'dm'), None, 'tp')
All inputs are finite; a program needn't handle non-finite values.
Results may differ from the reference program's by a relative error of at most 0.0107095.
Values are sent between devices in bfloat16 or wider.
A program may use at most 768 MiB of HBM per device.

```python
import math
import jax
import jax.numpy as jnp
from jax import lax

D = 4096
HEADS = 32
KV_HEADS = 32
HEAD = 128
FF = 11008
BATCH = 128
SEQ = 256

GROUP = HEADS // KV_HEADS
HALF = HEAD // 2
EPS = 1e-6
ROPE_BASE = 10000.0
K_SCALE = math.sqrt(max(math.log(SEQ / 16.0), 1.0))


def rope_tables(seq_lens):
    inv_freq = ROPE_BASE ** (-2.0 * jnp.arange(HALF, dtype=jnp.float32) / HEAD)
    angles = seq_lens.astype(jnp.float32)[:, None] * inv_freq[None, :]
    return jnp.cos(angles), jnp.sin(angles)


def draw_lengths(key):
    lengths = jax.random.randint(key, (BATCH,), SEQ // 8, SEQ, dtype=jnp.int32)
    return lengths.at[0].set(SEQ - 1).at[BATCH - 1].set(SEQ // 8)


def setup_inputs(seed: int = 0, part: int = 0) -> dict:
    shared = jax.random.split(jax.random.key(seed), 9)
    local = jax.random.split(jax.random.fold_in(jax.random.key(seed), part), 4)
    w_q = (jax.random.normal(shared[0], (D, HEADS, HEAD), jnp.float32) * D ** -0.5).astype(jnp.bfloat16)
    w_k = (jax.random.normal(shared[1], (D, KV_HEADS, HEAD), jnp.float32) * (K_SCALE * D ** -0.5)).astype(jnp.bfloat16)
    w_v = (jax.random.normal(shared[2], (D, KV_HEADS, HEAD), jnp.float32) * D ** -0.5).astype(jnp.bfloat16)
    w_o = (jax.random.normal(shared[3], (HEADS, HEAD, D), jnp.float32) * (HEADS * HEAD) ** -0.5).astype(jnp.bfloat16)
    w_gate = (jax.random.normal(shared[4], (D, FF), jnp.float32) * D ** -0.5).astype(jnp.bfloat16)
    w_up = (jax.random.normal(shared[5], (D, FF), jnp.float32) * D ** -0.5).astype(jnp.bfloat16)
    w_down = (jax.random.normal(shared[6], (FF, D), jnp.float32) * FF ** -0.5).astype(jnp.bfloat16)
    norm_attn = (1.0 + 0.4 * jax.random.normal(shared[7], (D,), jnp.float32)).astype(jnp.bfloat16)
    norm_mlp = (1.0 + 0.4 * jax.random.normal(shared[8], (D,), jnp.float32)).astype(jnp.bfloat16)
    hidden = jax.random.normal(local[0], (BATCH, D), jnp.float32).astype(jnp.bfloat16)
    k_cache = (jax.random.normal(local[1], (BATCH, SEQ, KV_HEADS, HEAD), jnp.float32) * K_SCALE).astype(jnp.bfloat16)
    v_cache = jax.random.normal(local[2], (BATCH, SEQ, KV_HEADS, HEAD), jnp.float32).astype(jnp.bfloat16)
    seq_lens = draw_lengths(local[3])
    rope_cos, rope_sin = rope_tables(seq_lens)
    return dict(hidden=hidden, w_q=w_q, w_k=w_k, w_v=w_v, w_o=w_o, w_gate=w_gate, w_up=w_up, w_down=w_down, norm_attn=norm_attn, norm_mlp=norm_mlp, k_cache=k_cache, v_cache=v_cache, seq_lens=seq_lens, rope_cos=rope_cos, rope_sin=rope_sin)


def rms_norm(x, gain):
    x_f32 = x.astype(jnp.float32)
    scale = lax.rsqrt(jnp.mean(x_f32 * x_f32, axis=-1, keepdims=True) + EPS)
    return (x_f32 * scale * gain.astype(jnp.float32)).astype(jnp.bfloat16)


def apply_rope(x, rope_cos, rope_sin):
    first = x[..., :HALF]
    second = x[..., HALF:]
    cosine = rope_cos[:, None, :]
    sine = rope_sin[:, None, :]
    return jnp.concatenate([first * cosine - second * sine, second * cosine + first * sine], axis=-1).astype(jnp.bfloat16)


def project(x, weight):
    return jnp.dot(x, weight.reshape(D, -1), preferred_element_type=jnp.float32).reshape(BATCH, -1, HEAD)


def attend_row(row_args):
    q_row, k_row, v_row, length = row_args
    q_grp = q_row.reshape(KV_HEADS, GROUP, HEAD).astype(jnp.float32)
    scores = jnp.einsum('kgd,skd->kgs', q_grp, k_row.astype(jnp.float32)) / math.sqrt(HEAD)
    key_mask = jnp.arange(SEQ)[None, None, :] <= length
    scores = jnp.where(key_mask, scores, -1e30)
    attn_probs = jax.nn.softmax(scores, axis=-1).astype(jnp.bfloat16).astype(jnp.float32)
    heads = jnp.einsum('kgs,skd->kgd', attn_probs, v_row.astype(jnp.float32))
    return heads.reshape(HEADS, HEAD).astype(jnp.bfloat16)


def reference(hidden, w_q, w_k, w_v, w_o, w_gate, w_up, w_down, norm_attn, norm_mlp, k_cache, v_cache, seq_lens, rope_cos, rope_sin):
    x_norm = rms_norm(hidden, norm_attn)
    q_rot = apply_rope(project(x_norm, w_q), rope_cos, rope_sin)
    k_rot = apply_rope(project(x_norm, w_k), rope_cos, rope_sin)
    v_new = project(x_norm, w_v).astype(jnp.bfloat16)
    write_mask = (jnp.arange(SEQ)[None, :] == seq_lens[:, None])[:, :, None, None]
    k_out = jnp.where(write_mask, k_rot[:, None], k_cache)
    v_out = jnp.where(write_mask, v_new[:, None], v_cache)
    attn_heads = lax.map(attend_row, (q_rot, k_out, v_out, seq_lens))
    attn_out = jnp.dot(attn_heads.reshape(BATCH, HEADS * HEAD), w_o.reshape(HEADS * HEAD, D), preferred_element_type=jnp.float32).astype(jnp.bfloat16)
    h_mid = hidden + attn_out
    x_mlp = rms_norm(h_mid, norm_mlp)
    gate = jnp.dot(x_mlp, w_gate, preferred_element_type=jnp.float32)
    up_proj = jnp.dot(x_mlp, w_up, preferred_element_type=jnp.float32)
    gated_act = (jax.nn.silu(gate) * up_proj).astype(jnp.bfloat16)
    mlp_out = jnp.dot(gated_act, w_down, preferred_element_type=jnp.float32).astype(jnp.bfloat16)
    return (h_mid + mlp_out, k_out, v_out)
```

```python
import functools

import jax
import jax.numpy as jnp
from jax import lax
from jax.experimental import pallas as pl
from jax.experimental.pallas import tpu as pltpu
from jax.sharding import PartitionSpec as P

EPS = 1e-6
MESH = pl.DeviceIdType.MESH
F32 = jnp.float32
BF16 = jnp.bfloat16
NT_DIMS = (((1,), (1,)), ((), ()))
TN_DIMS = (((0,), (0,)), ((), ()))


def remote(src, dst, send_sem, recv_sem, axis, index):
    return pltpu.make_async_remote_copy(
        src_ref=src, dst_ref=dst, send_sem=send_sem, recv_sem=recv_sem,
        device_id={axis: index}, device_id_type=MESH)


def meet(axes):
    barrier = pltpu.get_barrier_semaphore()
    total = 0
    for axis, n in axes:
        me = lax.axis_index(axis)
        for rel in range(1, n):
            pl.semaphore_signal(barrier, inc=1, device_id={axis: lax.rem(me + rel, n)}, device_id_type=MESH)
        total += n - 1
    pl.semaphore_wait(barrier, total)


def column_to_row(col, lanes):
    rows = col.shape[0]
    r = lax.broadcasted_iota(jnp.int32, (rows, lanes), 0)
    c = lax.broadcasted_iota(jnp.int32, (rows, lanes), 1)
    return jnp.sum(jnp.where(r == c, jnp.broadcast_to(col, (rows, lanes)), 0.0), axis=0, keepdims=True)


def row_to_column(row, rows):
    lanes = row.shape[1]
    r = lax.broadcasted_iota(jnp.int32, (rows, lanes), 0)
    c = lax.broadcasted_iota(jnp.int32, (rows, lanes), 1)
    return jnp.sum(jnp.where(r == c, jnp.broadcast_to(row, (rows, lanes)), 0.0), axis=1, keepdims=True)


def qkv_kernel(nd, heads, width_full, hid_ref, gain_ref, wq_ref, wk_ref, wv_ref, cos_ref, sin_ref,
               q_out, k_out, v_out,
               wbuf, w32, wcat, stat, part, sbuf, rbuf,
               wsem, st_ss, st_rs, ss, rs):
    me = lax.axis_index('dm')
    batch, width = hid_ref.shape
    rows = batch // nd
    cols = wcat.shape[2]
    loads = [pltpu.make_async_copy(w, wbuf.at[j], wsem.at[j]) for j, w in enumerate((wq_ref, wk_ref, wv_ref))]
    for load in loads:
        load.start()
    x = hid_ref[...].astype(F32)
    stat[me] = column_to_row(jnp.sum(x * x, axis=1, keepdims=True), batch)
    meet((('dm', nd),))
    st_copies = [remote(stat.at[me], stat.at[me], st_ss.at[rel], st_rs.at[rel], 'dm', lax.rem(me + rel, nd)) for rel in range(1, nd)]
    for copy in st_copies:
        copy.start()
    step = width // 8
    for j in range(3):
        loads[j].wait()

        @pl.loop(0, 8)
        def _(c, j=j):
            src = pl.multiple_of(c * step * heads, step * heads)
            w32[...] = wbuf[j, pl.ds(src, step * heads), :].astype(F32)
            dst = pl.multiple_of(c * step, step)
            for h in range(heads):
                wcat[j, pl.ds(dst, step), h * 128:(h + 1) * 128] = w32[pl.ds(h, step, stride=heads), :].astype(BF16)
    for copy in st_copies:
        copy.wait()
    total = stat[0]
    for i in range(1, nd):
        total = total + stat[i]
    scale = lax.rsqrt(row_to_column(total, batch) / width_full + EPS)
    gain = gain_ref[...].astype(F32)
    x_norm = (x * scale * gain).astype(BF16)
    copies = []
    for j in range(3):
        out = jnp.dot(x_norm, wcat[j], preferred_element_type=F32)
        for i in range(nd):
            part[j, i] = out[i * rows:(i + 1) * rows]
            sbuf[j, i] = out[i * rows:(i + 1) * rows].astype(BF16)
        for rel in (2, 1, 3) if nd == 4 else range(1, nd):
            to = lax.rem(me + rel, nd)
            copy = remote(sbuf.at[j, to], rbuf.at[j, me], ss.at[j, rel], rs.at[j, rel], 'dm', to)
            copy.start()
            copies.append(copy)
    cos = cos_ref[...]
    sin = sin_ref[...]
    cos = jnp.concatenate([cos, cos], axis=1)
    sin = jnp.concatenate([-sin, sin], axis=1)
    for j in range(3):
        for copy in copies[j * (nd - 1):(j + 1) * (nd - 1)]:
            copy.wait_recv()
        total = part[j, me]
        for rel in range(1, nd):
            total = total + rbuf[j, lax.rem(me + nd - rel, nd)].astype(F32)
        for h in range(heads):
            v = total[:, h * 128:(h + 1) * 128]
            if j < 2:
                v = v * cos + pltpu.roll(v, 64, 1) * sin
            v = v.astype(BF16).astype(F32)
            if j == 0:
                q_out[:, h] = v.reshape(rows // 8, 8, 128)
            elif j == 1:
                k_out[h] = v
            else:
                v_out[h] = v
    for copy in copies:
        copy.wait_send()


def attend_kernel(len_ref, q_ref, knew_ref, vnew_ref, k_hbm, v_hbm, o_ref, k_hbm_out, v_hbm_out,
                  k_buf, v_buf, new, new16, o32, in_sem, out_sem):
    groups, heads, gb, dim = q_ref.shape
    rows, span, _ = k_hbm.shape

    def copy_in(g, j):
        at = pl.ds(g * gb, gb)
        return pltpu.make_async_copy((k_hbm, v_hbm)[j].at[at], (k_buf, v_buf)[j].at[at], in_sem.at[j, g])

    def copy_out(g, j):
        at = pl.ds(g * gb, gb)
        return pltpu.make_async_copy((k_buf, v_buf)[j].at[at], (k_hbm_out, v_hbm_out)[j].at[at], out_sem.at[j, g])

    for g in range(groups):
        for j in range(2):
            copy_in(g, j).start()
    lane = lax.broadcasted_iota(jnp.int32, (heads * gb, span), 1)
    row = lax.broadcasted_iota(jnp.int32, (heads * gb, span), 0)
    head_ok = lane % heads == row // gb
    slot = lane // heads
    row1 = lax.broadcasted_iota(jnp.int32, (heads * gb, 128), 0)
    r16 = lax.broadcasted_iota(jnp.int32, (16, 128), 0) // heads
    per = 16 // heads
    for j, src in enumerate((knew_ref, vnew_ref)):
        for h in range(heads):
            for s in range(per):
                new[pl.ds(s * heads + h, rows, stride=16), :] = src[h]
        new16[j] = new[...].astype(BF16)

    @pl.loop(0, groups)
    def _(g):
        for j in range(2):
            copy_in(g, j).wait()
        lens = jnp.zeros((heads * gb, 128), jnp.int32)
        for b8 in range(gb):
            b = g * gb + b8
            n = len_ref[b]
            lens = jnp.where(row1 % gb == b8, n, lens)
            at = pl.ds(pl.multiple_of((n // per) * 16, 16), 16)
            hit = r16 == n % per
            src = pl.ds(pl.multiple_of(b * 16, 16), 16)
            for j, cache in enumerate((k_buf, v_buf)):
                old = cache[b, at, :].astype(F32)
                cache[b, at, :] = jnp.where(hit, new16[j, src, :].astype(F32), old).astype(BF16)
        q = jnp.concatenate([q_ref[g, h] for h in range(heads)], axis=0)
        q_exp = jnp.concatenate([jnp.where(row1 % gb == b8, q, 0.0).astype(BF16) for b8 in range(gb)], axis=1)
        parts = []
        for nb in range(span // 256):
            keys = jnp.concatenate([k_buf[g * gb + b8, nb * 256:(nb + 1) * 256, :] for b8 in range(gb)], axis=1)
            parts.append(lax.dot_general(q_exp, keys, NT_DIMS, preferred_element_type=F32))
        s = jnp.concatenate(parts, axis=1) * (dim ** -0.5)
        ok = head_ok & (slot <= jnp.concatenate([lens] * (span // 128), axis=1))
        s = jnp.where(ok, s, -1e30)
        top = jnp.max(s, axis=1, keepdims=True)
        e = jnp.where(ok, jnp.exp(s - top), 0.0)
        p = (e / jnp.sum(e, axis=1, keepdims=True))
        acc = jnp.zeros((heads * gb, 2 * dim), F32)
        half = gb // 2
        for pair in range(half):
            p_pair = jnp.where(row % half == pair, p, 0.0).astype(BF16)
            vals = jnp.concatenate([v_buf[g * gb + pair], v_buf[g * gb + pair + half]], axis=1)
            acc = acc + jnp.dot(p_pair, vals, preferred_element_type=F32)
        o = jnp.where(row1 % gb < half, acc[:, :dim], acc[:, dim:])
        for h in range(heads):
            o32[pl.ds(pl.multiple_of(g * gb, gb), gb), h * dim:(h + 1) * dim] = o[h * gb:(h + 1) * gb]
        for j in range(2):
            copy_out(g, j).start()

    o_ref[...] = o32[...].astype(BF16)
    for g in range(groups):
        for j in range(2):
            copy_out(g, j).wait()


def mlp_kernel(nd, nt, fc, width_full, o_ref, hid_ref, gain_ref, wo_hbm, wg_hbm, wu_hbm, wd_hbm, out_ref,
               wo, wg, wu, wd, o_all, acc32, rs1_s, rs1_r, mid, st_dm, st_tp, x2, gu_s, gu_r, gu_own, m_all,
               rs2_s, rs2_r, fin,
               wsem, o_ss, o_rs, a_ss, a_rs, b_ss, b_rs, sd_ss, sd_rs, st_ss, st_rs, g_ss, g_rs, m_ss, m_rs,
               c_ss, c_rs, d_ss, d_rs):
    dm = lax.axis_index('dm')
    tp = lax.axis_index('tp')
    rows_d = o_ref.shape[0]
    rows_t = mid.shape[1]
    per = rows_d // rows_t
    width = hid_ref.shape[1]
    ff = wg_hbm.shape[0]
    sends = []
    wloads = [pltpu.make_async_copy(wo_hbm, wo, wsem.at[0]),
              pltpu.make_async_copy(wg_hbm, wg.at[pl.ds(0, ff)], wsem.at[1]),
              pltpu.make_async_copy(wu_hbm, wu.at[pl.ds(0, ff)], wsem.at[2]),
              pltpu.make_async_copy(wd_hbm, wd.at[pl.ds(0, ff)], wsem.at[3])]
    for load in wloads:
        load.start()
    meet((('dm', nd), ('tp', nt)))
    o_copies = {}
    for rel in (2, 1, 3) if nd == 4 else range(1, nd):
        to = lax.rem(dm + rel, nd)
        o_copies[rel] = remote(o_ref, o_all.at[dm], o_ss.at[rel], o_rs.at[rel], 'dm', to)
        o_copies[rel].start()
        sends.append(o_copies[rel])
    if wg.shape[0] > ff:
        for w in (wg, wu, wd):
            w[ff:, :] = jnp.zeros((w.shape[0] - ff, width), BF16)
    wloads[0].wait()
    for rel in range(nd):
        j = lax.rem(dm + nd - rel, nd)
        if rel:
            o_copies[rel].wait_recv()
            o = o_all[j]
        else:
            o = o_ref[...]
        part = jnp.dot(o, wo[...], preferred_element_type=F32)
        for c in range(per):
            t = j * per + c
            acc32[t] = part[c * rows_t:(c + 1) * rows_t]
            rs1_s[t] = part[c * rows_t:(c + 1) * rows_t].astype(BF16)
            far = lax.rem(t + nt - tp, nt)

            @pl.when(far != 0)
            def _(t=t, far=far):
                remote(rs1_s.at[t], rs1_r.at[tp], a_ss.at[far], a_rs.at[far], 'tp', t).start()

    def reduced(acc, recv, s_sems, r_sems, sent):
        total = acc[tp]
        for rel in range(1, nt):
            frm = lax.rem(tp + nt - rel, nt)
            copy = remote(sent.at[frm], recv.at[frm], s_sems.at[rel], r_sems.at[rel], 'tp', frm)
            copy.wait_recv()
            total = total + recv[frm].astype(F32)
            sends.append(copy)
        return total.astype(BF16)

    def gather(buf, s_sems, r_sems):
        out = {}
        for rel in range(1, nt):
            out[rel] = remote(buf.at[tp], buf.at[tp], s_sems.at[rel], r_sems.at[rel], 'tp', lax.rem(tp + rel, nt))
            out[rel].start()
            sends.append(out[rel])
        return out

    attn = reduced(acc32, rs1_r, a_ss, a_rs, rs1_s)
    hid = hid_ref[pl.ds(pl.multiple_of(tp * rows_t, rows_t), rows_t), :]
    mine = (hid.astype(F32) + attn.astype(F32)).astype(BF16)
    mid[tp] = mine
    mid_copies = gather(mid, b_ss, b_rs)
    y = mine.astype(F32)
    st_dm[dm] = column_to_row(jnp.sum(y * y, axis=1, keepdims=True), 128)
    sd_copies = []
    for rel in range(1, nd):
        copy = remote(st_dm.at[dm], st_dm.at[dm], sd_ss.at[rel], sd_rs.at[rel], 'dm', lax.rem(dm + rel, nd))
        copy.start()
        sd_copies.append(copy)
    sends.extend(sd_copies)
    for copy in sd_copies:
        copy.wait_recv()
    total = st_dm[0]
    for i in range(1, nd):
        total = total + st_dm[i]
    st_tp[tp] = total
    st_copies = gather(st_tp, st_ss, st_rs)
    gain = gain_ref[...].astype(F32)
    for rel in range(nt):
        t = lax.rem(tp + nt - rel, nt)
        if rel:
            st_copies[rel].wait_recv()
            mid_copies[rel].wait_recv()
        scale = lax.rsqrt(row_to_column(st_tp[t], rows_t) / width_full + EPS)
        x2[pl.ds(pl.multiple_of(t * rows_t, rows_t), rows_t), :] = (mid[t].astype(F32) * scale * gain).astype(BF16)
    wloads[1].wait()
    wloads[2].wait()
    g_copies = {}
    for rel in (2, 1, 3, 0) if nd == 4 else [*range(1, nd), 0]:
        to = lax.rem(dm + rel, nd)
        at = pl.ds(pl.multiple_of(to * fc, 16), fc)
        for i, w in enumerate((wg, wu)):
            part = lax.dot_general(w[at, :], x2[...], NT_DIMS, preferred_element_type=F32)
            if rel:
                gu_s[to, i] = part.astype(BF16)
            else:
                gu_own[i] = part
        if rel:
            g_copies[rel] = remote(gu_s.at[to], gu_r.at[dm], g_ss.at[rel], g_rs.at[rel], 'dm', to)
            g_copies[rel].start()
            sends.append(g_copies[rel])
    gate = gu_own[0]
    up = gu_own[1]
    for rel in (1, 3, 2) if nd == 4 else range(1, nd):
        frm = lax.rem(dm + nd - rel, nd)
        g_copies[rel].wait_recv()
        gate = gate + gu_r[frm, 0].astype(F32)
        up = up + gu_r[frm, 1].astype(F32)
    m_all[dm] = (gate / (1.0 + jnp.exp(-gate)) * up).astype(BF16)
    m_copies = {}
    for rel in (2, 1, 3) if nd == 4 else range(1, nd):
        m_copies[rel] = remote(m_all.at[dm], m_all.at[dm], m_ss.at[rel], m_rs.at[rel], 'dm', lax.rem(dm + rel, nd))
        m_copies[rel].start()
        sends.append(m_copies[rel])
    wloads[3].wait()
    for k, rel in enumerate((0, 1, 3, 2) if nd == 4 else range(nd)):
        j = lax.rem(dm + nd - rel, nd)
        if rel:
            m_copies[rel].wait_recv()
        part = lax.dot_general(m_all[j], wd[pl.ds(pl.multiple_of(j * fc, 16), fc), :], TN_DIMS, preferred_element_type=F32)
        for t in range(nt):
            piece = part[t * rows_t:(t + 1) * rows_t]
            acc32[t] = piece if k == 0 else acc32[t] + piece
    for t in range(nt):
        rs2_s[t] = acc32[t].astype(BF16)
    for rel in range(1, nt):
        to = lax.rem(tp + rel, nt)
        remote(rs2_s.at[to], rs2_r.at[tp], c_ss.at[rel], c_rs.at[rel], 'tp', to).start()
    mlp = reduced(acc32, rs2_r, c_ss, c_rs, rs2_s)
    fin[tp] = (mid[tp].astype(F32) + mlp.astype(F32)).astype(BF16)
    f_copies = gather(fin, d_ss, d_rs)
    for rel in range(nt):
        t = lax.rem(tp + nt - rel, nt)
        if rel:
            f_copies[rel].wait_recv()
        out_ref[pl.ds(pl.multiple_of(t * rows_t, rows_t), rows_t), :] = fin[t]
    for copy in sends:
        copy.wait_send()


VMEM = pl.BlockSpec(memory_space=pltpu.VMEM)
SMEM = pl.BlockSpec(memory_space=pltpu.SMEM)
HBM = pl.BlockSpec(memory_space=pltpu.HBM)
MIB = 1 << 20


def solution(mesh):
    nd = mesh.shape['dm']
    nt = mesh.shape['tp']
    row_spec = P('dp', 'dm')
    cache_spec = P(('dp', 'dm'), None, 'tp', None)
    batch_spec = P(('dp', 'dm'))
    rope_spec = P(('dp', 'dm'), None)
    in_specs = (row_spec, P('dm', 'tp', None), P('dm', 'tp', None), P('dm', 'tp', None), P('tp', None, 'dm'), P('dm', 'tp'), P('dm', 'tp'), P('tp', 'dm'), P('dm'), P('dm'), cache_spec, cache_spec, batch_spec, rope_spec, rope_spec)
    out_specs = (row_spec, cache_spec, cache_spec)
    dma = pltpu.SemaphoreType.DMA

    def local_layer(hidden, w_q, w_k, w_v, w_o, w_gate, w_up, w_down, norm_attn, norm_mlp, k_cache, v_cache, seq_lens, rope_cos, rope_sin):
        batch, width = hidden.shape
        width_full = width * nd
        _, heads, dim = w_q.shape
        rows, seq = k_cache.shape[:2]
        cols = heads * dim
        ff = w_gate.shape[1]
        def hbm(x):
            return pltpu.with_memory_space_constraint(x, pltpu.HBM)

        q, k, v = pl.pallas_call(
            functools.partial(qkv_kernel, nd, heads, width_full),
            out_shape=(jax.ShapeDtypeStruct((rows // 8, heads, 8, dim), F32),
                       jax.ShapeDtypeStruct((heads, rows, dim), F32),
                       jax.ShapeDtypeStruct((heads, rows, dim), F32)),
            in_specs=[VMEM, VMEM, HBM, HBM, HBM, VMEM, VMEM],
            out_specs=(VMEM, VMEM, VMEM),
            scratch_shapes=[
                pltpu.VMEM((3, width * heads, dim), BF16),
                pltpu.VMEM((width // 8 * heads, dim), F32),
                pltpu.VMEM((3, width, cols), BF16),
                pltpu.VMEM((nd, 1, batch), F32),
                pltpu.VMEM((3, nd, rows, cols), F32),
                pltpu.VMEM((3, nd, rows, cols), BF16),
                pltpu.VMEM((3, nd, rows, cols), BF16),
                dma((3,)), dma((nd,)), dma((nd,)), dma((3, nd)), dma((3, nd)),
            ],
            compiler_params=pltpu.CompilerParams(collective_id=0, has_side_effects=True, vmem_limit_bytes=16 * MIB),
            name='qkv',
        )(hidden, norm_attn.reshape(1, width), hbm(w_q.reshape(width * heads, dim)), hbm(w_k.reshape(width * heads, dim)),
          hbm(w_v.reshape(width * heads, dim)), rope_cos, rope_sin)

        flat = (rows, seq * heads, dim)
        o, k_new, v_new = pl.pallas_call(
            attend_kernel,
            out_shape=(jax.ShapeDtypeStruct((rows, cols), BF16),
                       jax.ShapeDtypeStruct(flat, BF16),
                       jax.ShapeDtypeStruct(flat, BF16)),
            in_specs=[SMEM, VMEM, VMEM, VMEM, HBM, HBM],
            out_specs=(VMEM, HBM, HBM),
            scratch_shapes=[
                pltpu.VMEM(flat, BF16),
                pltpu.VMEM(flat, BF16),
                pltpu.VMEM((rows * 16, dim), F32),
                pltpu.VMEM((2, rows * 16, dim), BF16),
                pltpu.VMEM((rows, cols), F32),
                dma((2, rows // 8)), dma((2, rows // 8)),
            ],
            compiler_params=pltpu.CompilerParams(vmem_limit_bytes=40 * MIB),
            name='attend',
        )(seq_lens, q, k, v, hbm(k_cache.reshape(flat)), hbm(v_cache.reshape(flat)))

        fc = -(-ff // (nd * 16)) * 16
        rows_t = batch // nt
        slab = (nt, rows_t, width)
        out = pl.pallas_call(
            functools.partial(mlp_kernel, nd, nt, fc, width_full),
            out_shape=jax.ShapeDtypeStruct((batch, width), BF16),
            in_specs=[VMEM, VMEM, VMEM, HBM, HBM, HBM, HBM],
            out_specs=VMEM,
            scratch_shapes=[
                pltpu.VMEM((cols, width), BF16),
                pltpu.VMEM((nd * fc, width), BF16),
                pltpu.VMEM((nd * fc, width), BF16),
                pltpu.VMEM((nd * fc, width), BF16),
                pltpu.VMEM((nd, rows, cols), BF16),
                pltpu.VMEM(slab, F32),
                pltpu.VMEM(slab, BF16),
                pltpu.VMEM(slab, BF16),
                pltpu.VMEM(slab, BF16),
                pltpu.VMEM((nd, 1, 128), F32),
                pltpu.VMEM((nt, 1, 128), F32),
                pltpu.VMEM((batch, width), BF16),
                pltpu.VMEM((nd, 2, fc, batch), BF16),
                pltpu.VMEM((nd, 2, fc, batch), BF16),
                pltpu.VMEM((2, fc, batch), F32),
                pltpu.VMEM((nd, fc, batch), BF16),
                pltpu.VMEM(slab, BF16),
                pltpu.VMEM(slab, BF16),
                pltpu.VMEM(slab, BF16),
                dma((4,)), dma((nd,)), dma((nd,)), dma((nt,)), dma((nt,)), dma((nt,)), dma((nt,)),
                dma((nd,)), dma((nd,)), dma((nt,)), dma((nt,)), dma((nd,)), dma((nd,)), dma((nd,)), dma((nd,)),
                dma((nt,)), dma((nt,)), dma((nt,)), dma((nt,)),
            ],
            compiler_params=pltpu.CompilerParams(collective_id=1, has_side_effects=True, vmem_limit_bytes=24 * MIB),
            name='mlp',
        )(o, hidden, norm_mlp.reshape(1, width), hbm(w_o.reshape(cols, width)), hbm(w_gate.T), hbm(w_up.T), hbm(w_down))
        return out, k_new.reshape(k_cache.shape), v_new.reshape(v_cache.shape)

    return jax.shard_map(local_layer, mesh=mesh, in_specs=in_specs, out_specs=out_specs, check_vma=False)
```

```python
import functools

import jax
import jax.numpy as jnp
from jax import lax
from jax.experimental import pallas as pl
from jax.experimental.pallas import tpu as pltpu
from jax.sharding import PartitionSpec as P

EPS = 1e-6
MESH = pl.DeviceIdType.MESH
F32 = jnp.float32
BF16 = jnp.bfloat16
NT_DIMS = (((1,), (1,)), ((), ()))
TN_DIMS = (((0,), (0,)), ((), ()))


def remote(src, dst, send_sem, recv_sem, axis, index):
    return pltpu.make_async_remote_copy(
        src_ref=src, dst_ref=dst, send_sem=send_sem, recv_sem=recv_sem,
        device_id={axis: index}, device_id_type=MESH)


def meet(axes):
    barrier = pltpu.get_barrier_semaphore()
    total = 0
    for axis, n in axes:
        me = lax.axis_index(axis)
        for rel in range(1, n):
            pl.semaphore_signal(barrier, inc=1, device_id={axis: lax.rem(me + rel, n)}, device_id_type=MESH)
        total += n - 1
    pl.semaphore_wait(barrier, total)


def column_to_row(col, lanes):
    rows = col.shape[0]
    r = lax.broadcasted_iota(jnp.int32, (rows, lanes), 0)
    c = lax.broadcasted_iota(jnp.int32, (rows, lanes), 1)
    return jnp.sum(jnp.where(r == c, jnp.broadcast_to(col, (rows, lanes)), 0.0), axis=0, keepdims=True)


def row_to_column(row, rows):
    lanes = row.shape[1]
    r = lax.broadcasted_iota(jnp.int32, (rows, lanes), 0)
    c = lax.broadcasted_iota(jnp.int32, (rows, lanes), 1)
    return jnp.sum(jnp.where(r == c, jnp.broadcast_to(row, (rows, lanes)), 0.0), axis=1, keepdims=True)


def qkv_kernel(nd, heads, width_full, hid_hbm, gain_hbm, wq_ref, wk_ref, wv_ref, cos_hbm, sin_hbm,
               q_out, k_out, v_out,
               hid_ref, gain_ref, cos_ref, sin_ref, wbuf, w32, wcat, stat, part, sbuf, rbuf,
               isem, wsem, st_ss, st_rs, ss, rs):
    me = lax.axis_index('dm')
    batch, width = hid_ref.shape
    rows = batch // nd
    small = [pltpu.make_async_copy(src, dst, isem.at[i]) for i, (src, dst) in enumerate(
        ((hid_hbm, hid_ref), (gain_hbm, gain_ref), (cos_hbm, cos_ref), (sin_hbm, sin_ref)))]
    for load in small:
        load.start()
    loads = [pltpu.make_async_copy(w, wbuf.at[j], wsem.at[j]) for j, w in enumerate((wq_ref, wk_ref, wv_ref))]
    for load in loads:
        load.start()
    for load in small:
        load.wait()
    x = hid_ref[...].astype(F32)
    stat[me] = column_to_row(jnp.sum(x * x, axis=1, keepdims=True), batch)
    meet((('dm', nd),))
    st_copies = [remote(stat.at[me], stat.at[me], st_ss.at[rel], st_rs.at[rel], 'dm', lax.rem(me + rel, nd)) for rel in range(1, nd)]
    for copy in st_copies:
        copy.start()
    step = width // 8
    for j in range(3):
        loads[j].wait()

        @pl.loop(0, 8)
        def _(c, j=j):
            src = pl.multiple_of(c * step * heads, step * heads)
            w32[...] = wbuf[j, pl.ds(src, step * heads), :].astype(F32)
            dst = pl.multiple_of(c * step, step)
            for h in range(heads):
                wcat[j, pl.ds(dst, step), h * 128:(h + 1) * 128] = w32[pl.ds(h, step, stride=heads), :].astype(BF16)
    for copy in st_copies:
        copy.wait()
    total = stat[0]
    for i in range(1, nd):
        total = total + stat[i]
    scale = lax.rsqrt(row_to_column(total, batch) / width_full + EPS)
    gain = gain_ref[...].astype(F32).reshape(1, width)
    x_norm = (x * scale * gain).astype(BF16)
    copies = []
    for j in range(3):
        out = jnp.dot(x_norm, wcat[j], preferred_element_type=F32)
        for i in range(nd):
            part[j, i] = out[i * rows:(i + 1) * rows]
            sbuf[j, i] = out[i * rows:(i + 1) * rows].astype(BF16)
        for rel in (2, 1, 3) if nd == 4 else range(1, nd):
            to = lax.rem(me + rel, nd)
            copy = remote(sbuf.at[j, to], rbuf.at[j, me], ss.at[j, rel], rs.at[j, rel], 'dm', to)
            copy.start()
            copies.append(copy)
    cos = cos_ref[...]
    sin = sin_ref[...]
    cos = jnp.concatenate([cos, cos], axis=1)
    sin = jnp.concatenate([-sin, sin], axis=1)
    for j in range(3):
        for copy in copies[j * (nd - 1):(j + 1) * (nd - 1)]:
            copy.wait_recv()
        total = part[j, me]
        for rel in range(1, nd):
            total = total + rbuf[j, lax.rem(me + nd - rel, nd)].astype(F32)
        for h in range(heads):
            v = total[:, h * 128:(h + 1) * 128]
            if j < 2:
                v = v * cos + pltpu.roll(v, 64, 1) * sin
            v = v.astype(BF16).astype(F32)
            if j == 0:
                q_out[:, h] = v.reshape(rows // 8, 8, 128)
            elif j == 1:
                k_out[h] = v
            else:
                v_out[h] = v
    for copy in copies:
        copy.wait_send()


def attend_kernel(len_ref, q_ref, knew_ref, vnew_ref, k_buf, v_buf, o_ref, k_out, v_out, new, patch, o32, out_sem, patch_sem):
    groups, heads, gb, dim = q_ref.shape
    rows, span, _ = k_buf.shape
    per = 16 // heads
    caches = ((k_buf, k_out), (v_buf, v_out))

    def bulk(g, j):
        at = pl.ds(g * gb, gb)
        return pltpu.make_async_copy(caches[j][0].at[at], caches[j][1].at[at], out_sem.at[j, g])

    def patch_copy(b, j):
        at = pl.ds(pl.multiple_of((len_ref[b] // per) * 16, 16), 16)
        return pltpu.make_async_copy(patch.at[j, b], caches[j][1].at[b, at], patch_sem.at[j, b])

    for g in range(groups):
        for j in range(2):
            bulk(g, j).start()
    lane = lax.broadcasted_iota(jnp.int32, (heads * gb, span), 1)
    row = lax.broadcasted_iota(jnp.int32, (heads * gb, span), 0)
    head_ok = lane % heads == row // gb
    slot = lane // heads
    row1 = lax.broadcasted_iota(jnp.int32, (heads * gb, dim), 0)
    r16 = lax.broadcasted_iota(jnp.int32, (16, dim), 0) // heads
    for j, src in enumerate((knew_ref, vnew_ref)):
        for h in range(heads):
            for s in range(per):
                new[j, pl.ds(s * heads + h, rows, stride=16), :] = src[h]

    @pl.loop(0, groups)
    def _(g):
        lens = jnp.zeros((heads * gb, dim), jnp.int32)
        for b8 in range(gb):
            b = g * gb + b8
            n = len_ref[b]
            lens = jnp.where(row1 % gb == b8, n, lens)
            at = pl.ds(pl.multiple_of((n // per) * 16, 16), 16)
            src = pl.ds(pl.multiple_of(b * 16, 16), 16)
            for j in range(2):
                old = caches[j][0][b, at, :].astype(F32)
                patch[j, b] = jnp.where(r16 == n % per, new[j, src, :], old).astype(BF16)
        mine = pl.ds(pl.multiple_of(g * gb, gb), gb)
        q = jnp.concatenate([q_ref[g, h] for h in range(heads)], axis=0)
        k_new = jnp.concatenate([knew_ref[h, mine, :] for h in range(heads)], axis=0)
        v_new = jnp.concatenate([vnew_ref[h, mine, :] for h in range(heads)], axis=0)
        q_exp = jnp.concatenate([jnp.where(row1 % gb == b8, q, 0.0).astype(BF16) for b8 in range(gb)], axis=1)
        parts = []
        for nb in range(span // 256):
            keys = jnp.concatenate([k_buf[g * gb + b8, nb * 256:(nb + 1) * 256, :] for b8 in range(gb)], axis=1)
            parts.append(lax.dot_general(q_exp, keys, NT_DIMS, preferred_element_type=F32))
        s = jnp.concatenate(parts, axis=1) * (dim ** -0.5)
        s_new = jnp.sum(q * k_new, axis=1, keepdims=True) * (dim ** -0.5)
        ok = head_ok & (slot < jnp.concatenate([lens] * (span // dim), axis=1))
        s = jnp.where(ok, s, -1e30)
        top = jnp.maximum(jnp.max(s, axis=1, keepdims=True), s_new)
        e = jnp.where(ok, jnp.exp(s - top), 0.0)
        e_new = jnp.exp(s_new - top)
        total = jnp.sum(e, axis=1, keepdims=True) + e_new
        p = e / total
        p_new = (e_new / total).astype(BF16).astype(F32)
        acc = jnp.zeros((heads * gb, 2 * dim), F32)
        half = gb // 2
        for pair in range(half):
            p_pair = jnp.where(row % half == pair, p, 0.0).astype(BF16)
            vals = jnp.concatenate([v_buf[g * gb + pair], v_buf[g * gb + pair + half]], axis=1)
            acc = acc + jnp.dot(p_pair, vals, preferred_element_type=F32)
        o = jnp.where(row1 % gb < half, acc[:, :dim], acc[:, dim:]) + p_new * v_new
        for h in range(heads):
            o32[mine, h * dim:(h + 1) * dim] = o[h * gb:(h + 1) * gb]
        for j in range(2):
            bulk(g, j).wait()
        for b8 in range(gb):
            for j in range(2):
                patch_copy(g * gb + b8, j).start()

    o_ref[...] = o32[...].astype(BF16)

    @pl.loop(0, rows)
    def _(b):
        for j in range(2):
            patch_copy(b, j).wait()


def mlp_kernel(nd, nt, fc, width_full, o_ref, hid_hbm, gain_hbm, wo_hbm, wg_hbm, wu_hbm, wd_hbm, out_ref,
               hid_ref, gain_ref, wo, wg, wu, wd, o_all, acc32, rs1_s, rs1_r, mid, st_dm, st_tp, x2, gu_s, gu_r, gu_own, m_all,
               rs2_s, rs2_r, fin,
               wsem, o_ss, o_rs, a_ss, a_rs, b_ss, b_rs, sd_ss, sd_rs, st_ss, st_rs, g_ss, g_rs, m_ss, m_rs,
               c_ss, c_rs, d_ss, d_rs):
    dm = lax.axis_index('dm')
    tp = lax.axis_index('tp')
    rows_d = o_ref.shape[0]
    rows_t = mid.shape[1]
    per = rows_d // rows_t
    width = hid_ref.shape[1]
    ff = wg_hbm.shape[0]
    sends = []
    wloads = [pltpu.make_async_copy(wo_hbm, wo, wsem.at[0]),
              pltpu.make_async_copy(wg_hbm, wg.at[pl.ds(0, ff)], wsem.at[1]),
              pltpu.make_async_copy(wu_hbm, wu.at[pl.ds(0, ff)], wsem.at[2]),
              pltpu.make_async_copy(wd_hbm, wd.at[pl.ds(0, ff)], wsem.at[3]),
              pltpu.make_async_copy(hid_hbm, hid_ref, wsem.at[4]),
              pltpu.make_async_copy(gain_hbm, gain_ref, wsem.at[5])]
    for load in wloads:
        load.start()
    meet((('dm', nd), ('tp', nt)))
    o_copies = {}
    for rel in (2, 1, 3) if nd == 4 else range(1, nd):
        to = lax.rem(dm + rel, nd)
        o_copies[rel] = remote(o_ref, o_all.at[dm], o_ss.at[rel], o_rs.at[rel], 'dm', to)
        o_copies[rel].start()
        sends.append(o_copies[rel])
    if wg.shape[0] > ff:
        for w in (wg, wu, wd):
            w[ff:, :] = jnp.zeros((w.shape[0] - ff, width), BF16)
    wloads[0].wait()
    for rel in range(nd):
        j = lax.rem(dm + nd - rel, nd)
        if rel:
            o_copies[rel].wait_recv()
            o = o_all[j]
        else:
            o = o_ref[...]
        part = jnp.dot(o, wo[...], preferred_element_type=F32)
        for c in range(per):
            t = j * per + c
            acc32[t] = part[c * rows_t:(c + 1) * rows_t]
            rs1_s[t] = part[c * rows_t:(c + 1) * rows_t].astype(BF16)
            far = lax.rem(t + nt - tp, nt)

            @pl.when(far != 0)
            def _(t=t, far=far):
                remote(rs1_s.at[t], rs1_r.at[tp], a_ss.at[far], a_rs.at[far], 'tp', t).start()

    def reduced(acc, recv, s_sems, r_sems, sent):
        total = acc[tp]
        for rel in range(1, nt):
            frm = lax.rem(tp + nt - rel, nt)
            copy = remote(sent.at[frm], recv.at[frm], s_sems.at[rel], r_sems.at[rel], 'tp', frm)
            copy.wait_recv()
            total = total + recv[frm].astype(F32)
            sends.append(copy)
        return total.astype(BF16)

    def gather(buf, s_sems, r_sems):
        out = {}
        for rel in range(1, nt):
            out[rel] = remote(buf.at[tp], buf.at[tp], s_sems.at[rel], r_sems.at[rel], 'tp', lax.rem(tp + rel, nt))
            out[rel].start()
            sends.append(out[rel])
        return out

    wloads[4].wait()
    wloads[5].wait()
    attn = reduced(acc32, rs1_r, a_ss, a_rs, rs1_s)
    hid = hid_ref[pl.ds(pl.multiple_of(tp * rows_t, rows_t), rows_t), :]
    mine = (hid.astype(F32) + attn.astype(F32)).astype(BF16)
    mid[tp] = mine
    mid_copies = gather(mid, b_ss, b_rs)
    y = mine.astype(F32)
    st_dm[dm] = column_to_row(jnp.sum(y * y, axis=1, keepdims=True), 128)
    sd_copies = []
    for rel in range(1, nd):
        copy = remote(st_dm.at[dm], st_dm.at[dm], sd_ss.at[rel], sd_rs.at[rel], 'dm', lax.rem(dm + rel, nd))
        copy.start()
        sd_copies.append(copy)
    sends.extend(sd_copies)
    for copy in sd_copies:
        copy.wait_recv()
    total = st_dm[0]
    for i in range(1, nd):
        total = total + st_dm[i]
    st_tp[tp] = total
    st_copies = gather(st_tp, st_ss, st_rs)
    gain = gain_ref[...].astype(F32).reshape(1, width)
    for rel in range(nt):
        t = lax.rem(tp + nt - rel, nt)
        if rel:
            st_copies[rel].wait_recv()
            mid_copies[rel].wait_recv()
        scale = lax.rsqrt(row_to_column(st_tp[t], rows_t) / width_full + EPS)
        x2[pl.ds(pl.multiple_of(t * rows_t, rows_t), rows_t), :] = (mid[t].astype(F32) * scale * gain).astype(BF16)
    wloads[1].wait()
    wloads[2].wait()
    g_copies = {}
    for rel in (2, 1, 3, 0) if nd == 4 else [*range(1, nd), 0]:
        to = lax.rem(dm + rel, nd)
        at = pl.ds(pl.multiple_of(to * fc, 16), fc)
        for i, w in enumerate((wg, wu)):
            part = lax.dot_general(w[at, :], x2[...], NT_DIMS, preferred_element_type=F32)
            if rel:
                gu_s[to, i] = part.astype(BF16)
            else:
                gu_own[i] = part
        if rel:
            g_copies[rel] = remote(gu_s.at[to], gu_r.at[dm], g_ss.at[rel], g_rs.at[rel], 'dm', to)
            g_copies[rel].start()
            sends.append(g_copies[rel])
    gate = gu_own[0]
    up = gu_own[1]
    for rel in (1, 3, 2) if nd == 4 else range(1, nd):
        frm = lax.rem(dm + nd - rel, nd)
        g_copies[rel].wait_recv()
        gate = gate + gu_r[frm, 0].astype(F32)
        up = up + gu_r[frm, 1].astype(F32)
    m_all[dm] = (gate / (1.0 + jnp.exp(-gate)) * up).astype(BF16)
    m_copies = {}
    for rel in (2, 1, 3) if nd == 4 else range(1, nd):
        m_copies[rel] = remote(m_all.at[dm], m_all.at[dm], m_ss.at[rel], m_rs.at[rel], 'dm', lax.rem(dm + rel, nd))
        m_copies[rel].start()
        sends.append(m_copies[rel])
    wloads[3].wait()
    for k, rel in enumerate((0, 1, 3, 2) if nd == 4 else range(nd)):
        j = lax.rem(dm + nd - rel, nd)
        if rel:
            m_copies[rel].wait_recv()
        part = lax.dot_general(m_all[j], wd[pl.ds(pl.multiple_of(j * fc, 16), fc), :], TN_DIMS, preferred_element_type=F32)
        for t in range(nt):
            piece = part[t * rows_t:(t + 1) * rows_t]
            acc32[t] = piece if k == 0 else acc32[t] + piece
    for t in range(nt):
        rs2_s[t] = acc32[t].astype(BF16)
    for rel in range(1, nt):
        to = lax.rem(tp + rel, nt)
        remote(rs2_s.at[to], rs2_r.at[tp], c_ss.at[rel], c_rs.at[rel], 'tp', to).start()
    mlp = reduced(acc32, rs2_r, c_ss, c_rs, rs2_s)
    fin[tp] = (mid[tp].astype(F32) + mlp.astype(F32)).astype(BF16)
    f_copies = gather(fin, d_ss, d_rs)
    for rel in range(nt):
        t = lax.rem(tp + nt - rel, nt)
        if rel:
            f_copies[rel].wait_recv()
        out_ref[pl.ds(pl.multiple_of(t * rows_t, rows_t), rows_t), :] = fin[t]
    for copy in sends:
        copy.wait_send()


VMEM = pl.BlockSpec(memory_space=pltpu.VMEM)
SEM = pl.BlockSpec(memory_space=pltpu.SEMAPHORE)
SMEM = pl.BlockSpec(memory_space=pltpu.SMEM)
HBM = pl.BlockSpec(memory_space=pltpu.HBM)
MIB = 1 << 20


def solution(mesh):
    nd = mesh.shape['dm']
    nt = mesh.shape['tp']
    row_spec = P('dp', 'dm')
    cache_spec = P(('dp', 'dm'), None, 'tp', None)
    batch_spec = P(('dp', 'dm'))
    rope_spec = P(('dp', 'dm'), None)
    in_specs = (row_spec, P('dm', 'tp', None), P('dm', 'tp', None), P('dm', 'tp', None), P('tp', None, 'dm'), P('dm', 'tp'), P('dm', 'tp'), P('tp', 'dm'), P('dm'), P('dm'), cache_spec, cache_spec, batch_spec, rope_spec, rope_spec)
    out_specs = (row_spec, cache_spec, cache_spec)
    dma = pltpu.SemaphoreType.DMA

    def local_layer(hidden, w_q, w_k, w_v, w_o, w_gate, w_up, w_down, norm_attn, norm_mlp, k_cache, v_cache, seq_lens, rope_cos, rope_sin):
        batch, width = hidden.shape
        width_full = width * nd
        _, heads, dim = w_q.shape
        rows, seq = k_cache.shape[:2]
        cols = heads * dim
        ff = w_gate.shape[1]
        def hbm(x):
            return pltpu.with_memory_space_constraint(x, pltpu.HBM)

        def vmem(x):
            return pltpu.with_memory_space_constraint(x, pltpu.VMEM)

        flat = (rows, seq * heads, dim)
        groups = rows // 8
        q, k, v = pl.pallas_call(
            functools.partial(qkv_kernel, nd, heads, width_full),
            out_shape=(jax.ShapeDtypeStruct((rows // 8, heads, 8, dim), F32),
                       jax.ShapeDtypeStruct((heads, rows, dim), F32),
                       jax.ShapeDtypeStruct((heads, rows, dim), F32)),
            in_specs=[HBM] * 7,
            out_specs=(VMEM, VMEM, VMEM),
            scratch_shapes=[
                pltpu.VMEM((batch, width), BF16),
                pltpu.VMEM((width,), BF16),
                pltpu.VMEM(rope_cos.shape, F32),
                pltpu.VMEM(rope_sin.shape, F32),
                pltpu.VMEM((3, width * heads, dim), BF16),
                pltpu.VMEM((width // 8 * heads, dim), F32),
                pltpu.VMEM((3, width, cols), BF16),
                pltpu.VMEM((nd, 1, batch), F32),
                pltpu.VMEM((3, nd, rows, cols), F32),
                pltpu.VMEM((3, nd, rows, cols), BF16),
                pltpu.VMEM((3, nd, rows, cols), BF16),
                dma((4,)), dma((3,)), dma((nd,)), dma((nd,)), dma((3, nd)), dma((3, nd)),
            ],
            compiler_params=pltpu.CompilerParams(collective_id=0, has_side_effects=True, vmem_limit_bytes=16 * MIB),
            cost_estimate=pl.CostEstimate(flops=10_000_000_000, bytes_accessed=32 * MIB, transcendentals=0),
            name='qkv',
        )(hbm(hidden), hbm(norm_attn), hbm(w_q.reshape(width * heads, dim)), hbm(w_k.reshape(width * heads, dim)),
          hbm(w_v.reshape(width * heads, dim)), hbm(rope_cos), hbm(rope_sin))

        o, k_new, v_new = pl.pallas_call(
            attend_kernel,
            out_shape=(jax.ShapeDtypeStruct((rows, cols), BF16), jax.ShapeDtypeStruct(flat, BF16), jax.ShapeDtypeStruct(flat, BF16)),
            in_specs=[SMEM, VMEM, VMEM, VMEM, VMEM, VMEM],
            out_specs=(VMEM, HBM, HBM),
            scratch_shapes=[
                pltpu.VMEM((2, rows * 16, dim), F32),
                pltpu.VMEM((2, rows, 16, dim), BF16),
                pltpu.VMEM((rows, cols), F32),
                dma((2, rows // 8)), dma((2, rows)),
            ],
            compiler_params=pltpu.CompilerParams(vmem_limit_bytes=8 * MIB),
            name='attend',
        )(seq_lens, q, k, v, vmem(k_cache.reshape(flat)), vmem(v_cache.reshape(flat)))

        fc = -(-ff // (nd * 16)) * 16
        rows_t = batch // nt
        slab = (nt, rows_t, width)
        out = pl.pallas_call(
            functools.partial(mlp_kernel, nd, nt, fc, width_full),
            out_shape=jax.ShapeDtypeStruct((batch, width), BF16),
            in_specs=[VMEM] + [HBM] * 6,
            out_specs=VMEM,
            scratch_shapes=[
                pltpu.VMEM((batch, width), BF16),
                pltpu.VMEM((width,), BF16),
                pltpu.VMEM((cols, width), BF16),
                pltpu.VMEM((nd * fc, width), BF16),
                pltpu.VMEM((nd * fc, width), BF16),
                pltpu.VMEM((nd * fc, width), BF16),
                pltpu.VMEM((nd, rows, cols), BF16),
                pltpu.VMEM(slab, F32),
                pltpu.VMEM(slab, BF16),
                pltpu.VMEM(slab, BF16),
                pltpu.VMEM(slab, BF16),
                pltpu.VMEM((nd, 1, 128), F32),
                pltpu.VMEM((nt, 1, 128), F32),
                pltpu.VMEM((batch, width), BF16),
                pltpu.VMEM((nd, 2, fc, batch), BF16),
                pltpu.VMEM((nd, 2, fc, batch), BF16),
                pltpu.VMEM((2, fc, batch), F32),
                pltpu.VMEM((nd, fc, batch), BF16),
                pltpu.VMEM(slab, BF16),
                pltpu.VMEM(slab, BF16),
                pltpu.VMEM(slab, BF16),
                dma((6,)), dma((nd,)), dma((nd,)), dma((nt,)), dma((nt,)), dma((nt,)), dma((nt,)),
                dma((nd,)), dma((nd,)), dma((nt,)), dma((nt,)), dma((nd,)), dma((nd,)), dma((nd,)), dma((nd,)),
                dma((nt,)), dma((nt,)), dma((nt,)), dma((nt,)),
            ],
            compiler_params=pltpu.CompilerParams(collective_id=1, has_side_effects=True, vmem_limit_bytes=24 * MIB),
            name='mlp',
        )(o, hbm(hidden), hbm(norm_mlp), hbm(w_o.reshape(cols, width)), hbm(w_gate.T), hbm(w_up.T), hbm(w_down))
        return out, k_new.reshape(k_cache.shape), v_new.reshape(v_cache.shape)

    return jax.shard_map(local_layer, mesh=mesh, in_specs=in_specs, out_specs=out_specs, check_vma=False)
```

```python
import functools

import jax
import jax.numpy as jnp
from jax import lax
from jax.experimental import pallas as pl
from jax.experimental.pallas import tpu as pltpu
from jax.sharding import PartitionSpec as P

EPS = 1e-6
MESH = pl.DeviceIdType.MESH
F32 = jnp.float32
BF16 = jnp.bfloat16
NT_DIMS = (((1,), (1,)), ((), ()))
TN_DIMS = (((0,), (0,)), ((), ()))


def remote(src, dst, send_sem, recv_sem, axis, index):
    return pltpu.make_async_remote_copy(
        src_ref=src, dst_ref=dst, send_sem=send_sem, recv_sem=recv_sem,
        device_id={axis: index}, device_id_type=MESH)


def meet(axes):
    barrier = pltpu.get_barrier_semaphore()
    total = 0
    for axis, n in axes:
        me = lax.axis_index(axis)
        for rel in range(1, n):
            pl.semaphore_signal(barrier, inc=1, device_id={axis: lax.rem(me + rel, n)}, device_id_type=MESH)
        total += n - 1
    pl.semaphore_wait(barrier, total)


def column_to_row(col, lanes):
    rows = col.shape[0]
    r = lax.broadcasted_iota(jnp.int32, (rows, lanes), 0)
    c = lax.broadcasted_iota(jnp.int32, (rows, lanes), 1)
    return jnp.sum(jnp.where(r == c, jnp.broadcast_to(col, (rows, lanes)), 0.0), axis=0, keepdims=True)


def row_to_column(row, rows):
    lanes = row.shape[1]
    r = lax.broadcasted_iota(jnp.int32, (rows, lanes), 0)
    c = lax.broadcasted_iota(jnp.int32, (rows, lanes), 1)
    return jnp.sum(jnp.where(r == c, jnp.broadcast_to(row, (rows, lanes)), 0.0), axis=1, keepdims=True)


def qkv_kernel(nd, heads, width_full, hid_hbm, gain_hbm, wq_ref, wk_ref, wv_ref, cos_hbm, sin_hbm,
               q_out, k_out, v_out,
               hid_ref, gain_ref, cos_ref, sin_ref, wbuf, w32, wcat, order, stat, part, sbuf, rbuf,
               isem, wsem, st_ss, st_rs, ss, rs):
    me = lax.axis_index('dm')
    batch, width = hid_ref.shape
    rows = batch // nd
    small = [pltpu.make_async_copy(src, dst, isem.at[i]) for i, (src, dst) in enumerate(
        ((hid_hbm, hid_ref), (gain_hbm, gain_ref), (cos_hbm, cos_ref), (sin_hbm, sin_ref)))]
    for load in small:
        load.start()
    loads = [pltpu.make_async_copy(w, wbuf.at[j], wsem.at[j]) for j, w in enumerate((wq_ref, wk_ref, wv_ref))]
    for load in loads:
        load.start()
    for load in small:
        load.wait()
    x = hid_ref[...].astype(F32)
    stat[me] = column_to_row(jnp.sum(x * x, axis=1, keepdims=True), batch)
    meet((('dm', nd),))
    st_copies = [remote(stat.at[me], stat.at[me], st_ss.at[rel], st_rs.at[rel], 'dm', lax.rem(me + rel, nd)) for rel in range(1, nd)]
    for copy in st_copies:
        copy.start()
    step = width // 8
    for j in range(3):
        loads[j].wait()

        @pl.loop(0, 8)
        def _(c, j=j):
            src = pl.multiple_of(c * step * heads, step * heads)
            w32[...] = wbuf[j, pl.ds(src, step * heads), :].astype(F32)
            dst = pl.multiple_of(c * step, step)
            for h in range(heads):
                wcat[j, pl.ds(dst, step), h * 128:(h + 1) * 128] = w32[pl.ds(h, step, stride=heads), :].astype(BF16)
    for copy in st_copies:
        copy.wait()
    total = stat[0]
    for i in range(1, nd):
        total = total + stat[i]
    scale = lax.rsqrt(row_to_column(total, batch) / width_full + EPS)
    gain = gain_ref[...].astype(F32).reshape(1, width)
    x_norm = (x * scale * gain).astype(BF16)
    copies = []
    for j in range(3):
        out = jnp.dot(x_norm, wcat[j], preferred_element_type=F32)
        for i in range(nd):
            part[j, i] = out[i * rows:(i + 1) * rows]
            sbuf[j, i] = out[i * rows:(i + 1) * rows].astype(BF16)
        for rel in (2, 1, 3) if nd == 4 else range(1, nd):
            to = lax.rem(me + rel, nd)
            copy = remote(sbuf.at[j, to], rbuf.at[j, me], ss.at[j, rel], rs.at[j, rel], 'dm', to)
            copy.start()
            copies.append(copy)
    cos = cos_ref[...]
    sin = sin_ref[...]
    cos = jnp.concatenate([cos, cos], axis=1)
    sin = jnp.concatenate([-sin, sin], axis=1)
    for j in range(3):
        for copy in copies[j * (nd - 1):(j + 1) * (nd - 1)]:
            copy.wait_recv()
        total = part[j, me]
        for rel in range(1, nd):
            total = total + rbuf[j, lax.rem(me + nd - rel, nd)].astype(F32)
        for h in range(heads):
            v = total[:, h * 128:(h + 1) * 128]
            if j < 2:
                v = v * cos + pltpu.roll(v, 64, 1) * sin
            v = v.astype(BF16).astype(F32)
            if j == 0:
                q_out[:, h] = v.reshape(rows // 8, 8, 128)
            else:
                order[pl.ds(h, rows, stride=heads), :] = v
        if j:
            (k_out, v_out)[j - 1][...] = order[...].astype(BF16)
    for copy in copies:
        copy.wait_send()


def attend_kernel(len_ref, q_ref, k_buf, v_buf, o_ref, o32):
    groups, heads, gb, dim = q_ref.shape
    rows, span, _ = k_buf.shape
    lane = lax.broadcasted_iota(jnp.int32, (heads * gb, span), 1)
    row = lax.broadcasted_iota(jnp.int32, (heads * gb, span), 0)
    head_ok = lane % heads == row // gb
    slot = lane // heads
    row1 = lax.broadcasted_iota(jnp.int32, (heads * gb, dim), 0)

    @pl.loop(0, groups)
    def _(g):
        lens = jnp.zeros((heads * gb, dim), jnp.int32)
        for b8 in range(gb):
            lens = jnp.where(row1 % gb == b8, len_ref[g * gb + b8], lens)
        mine = pl.ds(pl.multiple_of(g * gb, gb), gb)
        q = jnp.concatenate([q_ref[g, h] for h in range(heads)], axis=0)
        q_exp = jnp.concatenate([jnp.where(row1 % gb == b8, q, 0.0).astype(BF16) for b8 in range(gb)], axis=1)
        parts = []
        for nb in range(span // 256):
            keys = jnp.concatenate([k_buf[g * gb + b8, nb * 256:(nb + 1) * 256, :] for b8 in range(gb)], axis=1)
            parts.append(lax.dot_general(q_exp, keys, NT_DIMS, preferred_element_type=F32))
        s = jnp.concatenate(parts, axis=1) * (dim ** -0.5)
        ok = head_ok & (slot <= jnp.concatenate([lens] * (span // dim), axis=1))
        s = jnp.where(ok, s, -1e30)
        top = jnp.max(s, axis=1, keepdims=True)
        e = jnp.where(ok, jnp.exp(s - top), 0.0)
        p = e / jnp.sum(e, axis=1, keepdims=True)
        acc = jnp.zeros((heads * gb, 2 * dim), F32)
        half = gb // 2
        for pair in range(half):
            p_pair = jnp.where(row % half == pair, p, 0.0).astype(BF16)
            vals = jnp.concatenate([v_buf[g * gb + pair], v_buf[g * gb + pair + half]], axis=1)
            acc = acc + jnp.dot(p_pair, vals, preferred_element_type=F32)
        o = jnp.where(row1 % gb < half, acc[:, :dim], acc[:, dim:])
        for h in range(heads):
            o32[mine, h * dim:(h + 1) * dim] = o[h * gb:(h + 1) * gb]

    o_ref[...] = o32[...].astype(BF16)


def mlp_kernel(nd, nt, fc, width_full, o_ref, hid_hbm, gain_hbm, wo_hbm, wg_hbm, wu_hbm, wd_hbm, k_kept, v_kept, out_ref,
               hid_ref, gain_ref, wo, wg, wu, wd, o_all, acc32, rs1_s, rs1_r, mid, st_dm, st_tp, x2, gu_s, gu_r, gu_own, m_all,
               rs2_s, rs2_r, fin,
               wsem, o_ss, o_rs, a_ss, a_rs, b_ss, b_rs, sd_ss, sd_rs, st_ss, st_rs, g_ss, g_rs, m_ss, m_rs,
               c_ss, c_rs, d_ss, d_rs):
    del k_kept, v_kept
    dm = lax.axis_index('dm')
    tp = lax.axis_index('tp')
    rows_d = o_ref.shape[0]
    rows_t = mid.shape[1]
    per = rows_d // rows_t
    width = hid_ref.shape[1]
    ff = wg_hbm.shape[0]
    sends = []
    wloads = [pltpu.make_async_copy(wo_hbm, wo, wsem.at[0]),
              pltpu.make_async_copy(wg_hbm, wg.at[pl.ds(0, ff)], wsem.at[1]),
              pltpu.make_async_copy(wu_hbm, wu.at[pl.ds(0, ff)], wsem.at[2]),
              pltpu.make_async_copy(wd_hbm, wd.at[pl.ds(0, ff)], wsem.at[3]),
              pltpu.make_async_copy(hid_hbm, hid_ref, wsem.at[4]),
              pltpu.make_async_copy(gain_hbm, gain_ref, wsem.at[5])]
    for load in wloads:
        load.start()
    meet((('dm', nd), ('tp', nt)))
    o_copies = {}
    for rel in (2, 1, 3) if nd == 4 else range(1, nd):
        to = lax.rem(dm + rel, nd)
        o_copies[rel] = remote(o_ref, o_all.at[dm], o_ss.at[rel], o_rs.at[rel], 'dm', to)
        o_copies[rel].start()
        sends.append(o_copies[rel])
    if wg.shape[0] > ff:
        for w in (wg, wu, wd):
            w[ff:, :] = jnp.zeros((w.shape[0] - ff, width), BF16)
    wloads[0].wait()
    for rel in range(nd):
        j = lax.rem(dm + nd - rel, nd)
        if rel:
            o_copies[rel].wait_recv()
            o = o_all[j]
        else:
            o = o_ref[...]
        part = jnp.dot(o, wo[...], preferred_element_type=F32)
        for c in range(per):
            t = j * per + c
            acc32[t] = part[c * rows_t:(c + 1) * rows_t]
            rs1_s[t] = part[c * rows_t:(c + 1) * rows_t].astype(BF16)
            far = lax.rem(t + nt - tp, nt)

            @pl.when(far != 0)
            def _(t=t, far=far):
                remote(rs1_s.at[t], rs1_r.at[tp], a_ss.at[far], a_rs.at[far], 'tp', t).start()

    def reduced(acc, recv, s_sems, r_sems, sent):
        total = acc[tp]
        for rel in range(1, nt):
            frm = lax.rem(tp + nt - rel, nt)
            copy = remote(sent.at[frm], recv.at[frm], s_sems.at[rel], r_sems.at[rel], 'tp', frm)
            copy.wait_recv()
            total = total + recv[frm].astype(F32)
            sends.append(copy)
        return total.astype(BF16)

    def gather(buf, s_sems, r_sems):
        out = {}
        for rel in range(1, nt):
            out[rel] = remote(buf.at[tp], buf.at[tp], s_sems.at[rel], r_sems.at[rel], 'tp', lax.rem(tp + rel, nt))
            out[rel].start()
            sends.append(out[rel])
        return out

    wloads[4].wait()
    wloads[5].wait()
    attn = reduced(acc32, rs1_r, a_ss, a_rs, rs1_s)
    hid = hid_ref[pl.ds(pl.multiple_of(tp * rows_t, rows_t), rows_t), :]
    mine = (hid.astype(F32) + attn.astype(F32)).astype(BF16)
    mid[tp] = mine
    mid_copies = gather(mid, b_ss, b_rs)
    y = mine.astype(F32)
    st_dm[dm] = column_to_row(jnp.sum(y * y, axis=1, keepdims=True), 128)
    sd_copies = []
    for rel in range(1, nd):
        copy = remote(st_dm.at[dm], st_dm.at[dm], sd_ss.at[rel], sd_rs.at[rel], 'dm', lax.rem(dm + rel, nd))
        copy.start()
        sd_copies.append(copy)
    sends.extend(sd_copies)
    for copy in sd_copies:
        copy.wait_recv()
    total = st_dm[0]
    for i in range(1, nd):
        total = total + st_dm[i]
    st_tp[tp] = total
    st_copies = gather(st_tp, st_ss, st_rs)
    gain = gain_ref[...].astype(F32).reshape(1, width)
    for rel in range(nt):
        t = lax.rem(tp + nt - rel, nt)
        if rel:
            st_copies[rel].wait_recv()
            mid_copies[rel].wait_recv()
        scale = lax.rsqrt(row_to_column(st_tp[t], rows_t) / width_full + EPS)
        x2[pl.ds(pl.multiple_of(t * rows_t, rows_t), rows_t), :] = (mid[t].astype(F32) * scale * gain).astype(BF16)
    wloads[1].wait()
    wloads[2].wait()
    g_copies = {}
    for rel in (2, 1, 3, 0) if nd == 4 else [*range(1, nd), 0]:
        to = lax.rem(dm + rel, nd)
        at = pl.ds(pl.multiple_of(to * fc, 16), fc)
        for i, w in enumerate((wg, wu)):
            part = lax.dot_general(w[at, :], x2[...], NT_DIMS, preferred_element_type=F32)
            if rel:
                gu_s[to, i] = part.astype(BF16)
            else:
                gu_own[i] = part
        if rel:
            g_copies[rel] = remote(gu_s.at[to], gu_r.at[dm], g_ss.at[rel], g_rs.at[rel], 'dm', to)
            g_copies[rel].start()
            sends.append(g_copies[rel])
    gate = gu_own[0]
    up = gu_own[1]
    for rel in (1, 3, 2) if nd == 4 else range(1, nd):
        frm = lax.rem(dm + nd - rel, nd)
        g_copies[rel].wait_recv()
        gate = gate + gu_r[frm, 0].astype(F32)
        up = up + gu_r[frm, 1].astype(F32)
    m_all[dm] = (gate / (1.0 + jnp.exp(-gate)) * up).astype(BF16)
    m_copies = {}
    for rel in (2, 1, 3) if nd == 4 else range(1, nd):
        m_copies[rel] = remote(m_all.at[dm], m_all.at[dm], m_ss.at[rel], m_rs.at[rel], 'dm', lax.rem(dm + rel, nd))
        m_copies[rel].start()
        sends.append(m_copies[rel])
    wloads[3].wait()
    for k, rel in enumerate((0, 1, 3, 2) if nd == 4 else range(nd)):
        j = lax.rem(dm + nd - rel, nd)
        if rel:
            m_copies[rel].wait_recv()
        part = lax.dot_general(m_all[j], wd[pl.ds(pl.multiple_of(j * fc, 16), fc), :], TN_DIMS, preferred_element_type=F32)
        for t in range(nt):
            piece = part[t * rows_t:(t + 1) * rows_t]
            acc32[t] = piece if k == 0 else acc32[t] + piece
    for t in range(nt):
        rs2_s[t] = acc32[t].astype(BF16)
    for rel in range(1, nt):
        to = lax.rem(tp + rel, nt)
        remote(rs2_s.at[to], rs2_r.at[tp], c_ss.at[rel], c_rs.at[rel], 'tp', to).start()
    mlp = reduced(acc32, rs2_r, c_ss, c_rs, rs2_s)
    fin[tp] = (mid[tp].astype(F32) + mlp.astype(F32)).astype(BF16)
    f_copies = gather(fin, d_ss, d_rs)
    for rel in range(nt):
        t = lax.rem(tp + nt - rel, nt)
        if rel:
            f_copies[rel].wait_recv()
        out_ref[pl.ds(pl.multiple_of(t * rows_t, rows_t), rows_t), :] = fin[t]
    for copy in sends:
        copy.wait_send()


VMEM = pl.BlockSpec(memory_space=pltpu.VMEM)
SEM = pl.BlockSpec(memory_space=pltpu.SEMAPHORE)
SMEM = pl.BlockSpec(memory_space=pltpu.SMEM)
HBM = pl.BlockSpec(memory_space=pltpu.HBM)
MIB = 1 << 20


def solution(mesh):
    nd = mesh.shape['dm']
    nt = mesh.shape['tp']
    row_spec = P('dp', 'dm')
    cache_spec = P(('dp', 'dm'), None, 'tp', None)
    batch_spec = P(('dp', 'dm'))
    rope_spec = P(('dp', 'dm'), None)
    in_specs = (row_spec, P('dm', 'tp', None), P('dm', 'tp', None), P('dm', 'tp', None), P('tp', None, 'dm'), P('dm', 'tp'), P('dm', 'tp'), P('tp', 'dm'), P('dm'), P('dm'), cache_spec, cache_spec, batch_spec, rope_spec, rope_spec)
    out_specs = (row_spec, cache_spec, cache_spec)
    dma = pltpu.SemaphoreType.DMA

    def local_layer(hidden, w_q, w_k, w_v, w_o, w_gate, w_up, w_down, norm_attn, norm_mlp, k_cache, v_cache, seq_lens, rope_cos, rope_sin):
        batch, width = hidden.shape
        width_full = width * nd
        _, heads, dim = w_q.shape
        rows, seq = k_cache.shape[:2]
        cols = heads * dim
        ff = w_gate.shape[1]
        def hbm(x):
            return pltpu.with_memory_space_constraint(x, pltpu.HBM)

        def vmem(x):
            return pltpu.with_memory_space_constraint(x, pltpu.VMEM)

        flat = (rows, seq * heads, dim)
        groups = rows // 8
        q, k, v = pl.pallas_call(
            functools.partial(qkv_kernel, nd, heads, width_full),
            out_shape=(jax.ShapeDtypeStruct((rows // 8, heads, 8, dim), F32),
                       jax.ShapeDtypeStruct((rows * heads, dim), BF16),
                       jax.ShapeDtypeStruct((rows * heads, dim), BF16)),
            in_specs=[HBM] * 7,
            out_specs=(VMEM, VMEM, VMEM),
            scratch_shapes=[
                pltpu.VMEM((batch, width), BF16),
                pltpu.VMEM((width,), BF16),
                pltpu.VMEM(rope_cos.shape, F32),
                pltpu.VMEM(rope_sin.shape, F32),
                pltpu.VMEM((3, width * heads, dim), BF16),
                pltpu.VMEM((width // 8 * heads, dim), F32),
                pltpu.VMEM((3, width, cols), BF16),
                pltpu.VMEM((rows * heads, dim), F32),
                pltpu.VMEM((nd, 1, batch), F32),
                pltpu.VMEM((3, nd, rows, cols), F32),
                pltpu.VMEM((3, nd, rows, cols), BF16),
                pltpu.VMEM((3, nd, rows, cols), BF16),
                dma((4,)), dma((3,)), dma((nd,)), dma((nd,)), dma((3, nd)), dma((3, nd)),
            ],
            compiler_params=pltpu.CompilerParams(collective_id=0, has_side_effects=True, vmem_limit_bytes=16 * MIB),
            cost_estimate=pl.CostEstimate(flops=10_000_000_000, bytes_accessed=32 * MIB, transcendentals=0),
            name='qkv',
        )(hbm(hidden), hbm(norm_attn), hbm(w_q.reshape(width * heads, dim)), hbm(w_k.reshape(width * heads, dim)),
          hbm(w_v.reshape(width * heads, dim)), hbm(rope_cos), hbm(rope_sin))

        hit = (jnp.arange(seq)[None, :] == seq_lens[:, None])[:, :, None, None]
        k_new = jnp.where(hit, k.reshape(rows, 1, heads, dim), k_cache)
        v_new = jnp.where(hit, v.reshape(rows, 1, heads, dim), v_cache)
        k_kept = vmem(k_new.reshape(flat))
        v_kept = vmem(v_new.reshape(flat))
        o = pl.pallas_call(
            attend_kernel,
            out_shape=jax.ShapeDtypeStruct((rows, cols), BF16),
            in_specs=[SMEM, VMEM, VMEM, VMEM],
            out_specs=VMEM,
            scratch_shapes=[
                pltpu.VMEM((rows, cols), F32),
            ],
            compiler_params=pltpu.CompilerParams(vmem_limit_bytes=8 * MIB),
            name='attend',
        )(seq_lens, q, k_kept, v_kept)

        fc = -(-ff // (nd * 16)) * 16
        rows_t = batch // nt
        slab = (nt, rows_t, width)
        out = pl.pallas_call(
            functools.partial(mlp_kernel, nd, nt, fc, width_full),
            out_shape=jax.ShapeDtypeStruct((batch, width), BF16),
            in_specs=[VMEM] + [HBM] * 6 + [VMEM, VMEM],
            out_specs=VMEM,
            scratch_shapes=[
                pltpu.VMEM((batch, width), BF16),
                pltpu.VMEM((width,), BF16),
                pltpu.VMEM((cols, width), BF16),
                pltpu.VMEM((nd * fc, width), BF16),
                pltpu.VMEM((nd * fc, width), BF16),
                pltpu.VMEM((nd * fc, width), BF16),
                pltpu.VMEM((nd, rows, cols), BF16),
                pltpu.VMEM(slab, F32),
                pltpu.VMEM(slab, BF16),
                pltpu.VMEM(slab, BF16),
                pltpu.VMEM(slab, BF16),
                pltpu.VMEM((nd, 1, 128), F32),
                pltpu.VMEM((nt, 1, 128), F32),
                pltpu.VMEM((batch, width), BF16),
                pltpu.VMEM((nd, 2, fc, batch), BF16),
                pltpu.VMEM((nd, 2, fc, batch), BF16),
                pltpu.VMEM((2, fc, batch), F32),
                pltpu.VMEM((nd, fc, batch), BF16),
                pltpu.VMEM(slab, BF16),
                pltpu.VMEM(slab, BF16),
                pltpu.VMEM(slab, BF16),
                dma((6,)), dma((nd,)), dma((nd,)), dma((nt,)), dma((nt,)), dma((nt,)), dma((nt,)),
                dma((nd,)), dma((nd,)), dma((nt,)), dma((nt,)), dma((nd,)), dma((nd,)), dma((nd,)), dma((nd,)),
                dma((nt,)), dma((nt,)), dma((nt,)), dma((nt,)),
            ],
            compiler_params=pltpu.CompilerParams(collective_id=1, has_side_effects=True, vmem_limit_bytes=24 * MIB),
            cost_estimate=pl.CostEstimate(flops=40_000_000_000, bytes_accessed=12 * MIB, transcendentals=0),
            name='mlp',
        )(o, hbm(hidden), hbm(norm_mlp), hbm(w_o.reshape(cols, width)), hbm(w_gate.T), hbm(w_up.T), hbm(w_down), k_kept, v_kept)
        return out, k_new.reshape(k_cache.shape), v_new.reshape(v_cache.shape)

    return jax.shard_map(local_layer, mesh=mesh, in_specs=in_specs, out_specs=out_specs, check_vma=False)
```

```python
import functools

import jax
import jax.numpy as jnp
from jax import lax
from jax.experimental import pallas as pl
from jax.experimental.pallas import tpu as pltpu
from jax.sharding import PartitionSpec as P

EPS = 1e-6
MESH = pl.DeviceIdType.MESH
F32 = jnp.float32
BF16 = jnp.bfloat16
NT_DIMS = (((1,), (1,)), ((), ()))
TN_DIMS = (((0,), (0,)), ((), ()))


def remote(src, dst, send_sem, recv_sem, axis, index):
    return pltpu.make_async_remote_copy(
        src_ref=src, dst_ref=dst, send_sem=send_sem, recv_sem=recv_sem,
        device_id={axis: index}, device_id_type=MESH)


def meet(axes):
    barrier = pltpu.get_barrier_semaphore()
    total = 0
    for axis, n in axes:
        me = lax.axis_index(axis)
        for rel in range(1, n):
            pl.semaphore_signal(barrier, inc=1, device_id={axis: lax.rem(me + rel, n)}, device_id_type=MESH)
        total += n - 1
    pl.semaphore_wait(barrier, total)


def column_to_row(col, lanes):
    rows = col.shape[0]
    r = lax.broadcasted_iota(jnp.int32, (rows, lanes), 0)
    c = lax.broadcasted_iota(jnp.int32, (rows, lanes), 1)
    return jnp.sum(jnp.where(r == c, jnp.broadcast_to(col, (rows, lanes)), 0.0), axis=0, keepdims=True)


def row_to_column(row, rows):
    lanes = row.shape[1]
    r = lax.broadcasted_iota(jnp.int32, (rows, lanes), 0)
    c = lax.broadcasted_iota(jnp.int32, (rows, lanes), 1)
    return jnp.sum(jnp.where(r == c, jnp.broadcast_to(row, (rows, lanes)), 0.0), axis=1, keepdims=True)


def qkv_kernel(nd, heads, width_full, hid_hbm, gain_hbm, wq_ref, wk_ref, wv_ref, cos_hbm, sin_hbm,
               q_out, k_out, v_out,
               hid_ref, gain_ref, cos_ref, sin_ref, wbuf, w32, wcat, stat, part, sbuf, rbuf,
               isem, wsem, st_ss, st_rs, ss, rs):
    me = lax.axis_index('dm')
    batch, width = hid_ref.shape
    rows = batch // nd
    small = [pltpu.make_async_copy(src, dst, isem.at[i]) for i, (src, dst) in enumerate(
        ((hid_hbm, hid_ref), (gain_hbm, gain_ref), (cos_hbm, cos_ref), (sin_hbm, sin_ref)))]
    for load in small:
        load.start()
    loads = [pltpu.make_async_copy(w, wbuf.at[j], wsem.at[j]) for j, w in enumerate((wq_ref, wk_ref, wv_ref))]
    for load in loads:
        load.start()
    for load in small:
        load.wait()
    x = hid_ref[...].astype(F32)
    stat[me] = column_to_row(jnp.sum(x * x, axis=1, keepdims=True), batch)
    meet((('dm', nd),))
    st_copies = [remote(stat.at[me], stat.at[me], st_ss.at[rel], st_rs.at[rel], 'dm', lax.rem(me + rel, nd)) for rel in range(1, nd)]
    for copy in st_copies:
        copy.start()
    step = width // 8
    for j in range(3):
        loads[j].wait()

        @pl.loop(0, 8)
        def _(c, j=j):
            src = pl.multiple_of(c * step * heads, step * heads)
            w32[...] = wbuf[j, pl.ds(src, step * heads), :].astype(F32)
            dst = pl.multiple_of(c * step, step)
            for h in range(heads):
                wcat[j, pl.ds(dst, step), h * 128:(h + 1) * 128] = w32[pl.ds(h, step, stride=heads), :].astype(BF16)
    for copy in st_copies:
        copy.wait()
    total = stat[0]
    for i in range(1, nd):
        total = total + stat[i]
    scale = lax.rsqrt(row_to_column(total, batch) / width_full + EPS)
    gain = gain_ref[...].astype(F32).reshape(1, width)
    x_norm = (x * scale * gain).astype(BF16)
    copies = []
    for j in range(3):
        out = jnp.dot(x_norm, wcat[j], preferred_element_type=F32)
        for i in range(nd):
            part[j, i] = out[i * rows:(i + 1) * rows]
            sbuf[j, i] = out[i * rows:(i + 1) * rows].astype(BF16)
        for rel in (2, 1, 3) if nd == 4 else range(1, nd):
            to = lax.rem(me + rel, nd)
            copy = remote(sbuf.at[j, to], rbuf.at[j, me], ss.at[j, rel], rs.at[j, rel], 'dm', to)
            copy.start()
            copies.append(copy)
    cos = cos_ref[...]
    sin = sin_ref[...]
    cos = jnp.concatenate([cos, cos], axis=1)
    sin = jnp.concatenate([-sin, sin], axis=1)
    for j in range(3):
        for copy in copies[j * (nd - 1):(j + 1) * (nd - 1)]:
            copy.wait_recv()
        total = part[j, me]
        for rel in range(1, nd):
            total = total + rbuf[j, lax.rem(me + nd - rel, nd)].astype(F32)
        for h in range(heads):
            v = total[:, h * 128:(h + 1) * 128]
            if j < 2:
                v = v * cos + pltpu.roll(v, 64, 1) * sin
            v = v.astype(BF16).astype(F32)
            if j == 0:
                q_out[:, h] = v.reshape(rows // 8, 8, 128)
            elif j == 1:
                k_out[h] = v
            else:
                v_out[h] = v
    for copy in copies:
        copy.wait_send()


def attend_kernel(len_ref, q_ref, knew_ref, vnew_ref, k_buf, v_buf, o_ref, k_out, v_out, new, patch, o32, out_sem, patch_sem):
    groups, heads, gb, dim = q_ref.shape
    rows, span, _ = k_buf.shape
    per = 16 // heads
    caches = ((k_buf, k_out), (v_buf, v_out))

    def bulk(g, j):
        at = pl.ds(g * gb, gb)
        return pltpu.make_async_copy(caches[j][0].at[at], caches[j][1].at[at], out_sem.at[j, g])

    def patch_copy(b, j):
        at = pl.ds(pl.multiple_of((len_ref[b] // per) * 16, 16), 16)
        return pltpu.make_async_copy(patch.at[j, b], caches[j][1].at[b, at], patch_sem.at[j, b])

    for g in range(groups):
        for j in range(2):
            bulk(g, j).start()
    lane = lax.broadcasted_iota(jnp.int32, (heads * gb, span), 1)
    row = lax.broadcasted_iota(jnp.int32, (heads * gb, span), 0)
    head_ok = lane % heads == row // gb
    slot = lane // heads
    row1 = lax.broadcasted_iota(jnp.int32, (heads * gb, dim), 0)
    r16 = lax.broadcasted_iota(jnp.int32, (16, dim), 0) // heads
    for j, src in enumerate((knew_ref, vnew_ref)):
        for h in range(heads):
            for s in range(per):
                new[j, pl.ds(s * heads + h, rows, stride=16), :] = src[h]

    @pl.loop(0, groups)
    def _(g):
        lens = jnp.zeros((heads * gb, dim), jnp.int32)
        for b8 in range(gb):
            b = g * gb + b8
            n = len_ref[b]
            lens = jnp.where(row1 % gb == b8, n, lens)
            at = pl.ds(pl.multiple_of((n // per) * 16, 16), 16)
            src = pl.ds(pl.multiple_of(b * 16, 16), 16)
            for j in range(2):
                old = caches[j][0][b, at, :].astype(F32)
                patch[j, b] = jnp.where(r16 == n % per, new[j, src, :], old).astype(BF16)
        mine = pl.ds(pl.multiple_of(g * gb, gb), gb)
        q = jnp.concatenate([q_ref[g, h] for h in range(heads)], axis=0)
        k_new = jnp.concatenate([knew_ref[h, mine, :] for h in range(heads)], axis=0)
        v_new = jnp.concatenate([vnew_ref[h, mine, :] for h in range(heads)], axis=0)
        q_exp = jnp.concatenate([jnp.where(row1 % gb == b8, q, 0.0).astype(BF16) for b8 in range(gb)], axis=1)
        parts = []
        for nb in range(span // 256):
            keys = jnp.concatenate([k_buf[g * gb + b8, nb * 256:(nb + 1) * 256, :] for b8 in range(gb)], axis=1)
            parts.append(lax.dot_general(q_exp, keys, NT_DIMS, preferred_element_type=F32))
        s = jnp.concatenate(parts, axis=1) * (dim ** -0.5)
        s_new = jnp.sum(q * k_new, axis=1, keepdims=True) * (dim ** -0.5)
        ok = head_ok & (slot < jnp.concatenate([lens] * (span // dim), axis=1))
        s = jnp.where(ok, s, -1e30)
        top = jnp.maximum(jnp.max(s, axis=1, keepdims=True), s_new)
        e = jnp.where(ok, jnp.exp(s - top), 0.0)
        e_new = jnp.exp(s_new - top)
        total = jnp.sum(e, axis=1, keepdims=True) + e_new
        p = e / total
        p_new = (e_new / total).astype(BF16).astype(F32)
        acc = jnp.zeros((heads * gb, 2 * dim), F32)
        half = gb // 2
        for pair in range(half):
            p_pair = jnp.where(row % half == pair, p, 0.0).astype(BF16)
            vals = jnp.concatenate([v_buf[g * gb + pair], v_buf[g * gb + pair + half]], axis=1)
            acc = acc + jnp.dot(p_pair, vals, preferred_element_type=F32)
        o = jnp.where(row1 % gb < half, acc[:, :dim], acc[:, dim:]) + p_new * v_new
        for h in range(heads):
            o32[mine, h * dim:(h + 1) * dim] = o[h * gb:(h + 1) * gb]

    o_ref[...] = o32[...].astype(BF16)

    @pl.loop(0, groups)
    def _(g):
        for j in range(2):
            bulk(g, j).wait()
            for b8 in range(gb):
                patch_copy(g * gb + b8, j).start()

    @pl.loop(0, rows)
    def _(b):
        for j in range(2):
            patch_copy(b, j).wait()


def mlp_kernel(nd, nt, fc, width_full, o_ref, hid_hbm, gain_hbm, wo_hbm, wg_hbm, wu_hbm, wd_hbm, out_ref,
               hid_ref, gain_ref, wo, wg, wu, wd, o_all, acc32, rs1_s, rs1_r, mid, st_dm, st_tp, x2, gu_far, gu_relay, gu_s, gu_r, gu_own, m_all,
               rs2_s, rs2_r, fin,
               wsem, o_ss, o_rs, a_ss, a_rs, b_ss, b_rs, sd_ss, sd_rs, st_ss, st_rs, g_ss, g_rs, m_ss, m_rs,
               c_ss, c_rs, d_ss, d_rs):
    dm = lax.axis_index('dm')
    tp = lax.axis_index('tp')
    rows_d = o_ref.shape[0]
    rows_t = mid.shape[1]
    per = rows_d // rows_t
    width = hid_ref.shape[1]
    ff = wg_hbm.shape[0]
    sends = []
    wloads = [pltpu.make_async_copy(wo_hbm, wo, wsem.at[0]),
              pltpu.make_async_copy(wg_hbm, wg.at[pl.ds(0, ff)], wsem.at[1]),
              pltpu.make_async_copy(wu_hbm, wu.at[pl.ds(0, ff)], wsem.at[2]),
              pltpu.make_async_copy(wd_hbm, wd.at[pl.ds(0, ff)], wsem.at[3]),
              pltpu.make_async_copy(hid_hbm, hid_ref, wsem.at[4]),
              pltpu.make_async_copy(gain_hbm, gain_ref, wsem.at[5])]
    for load in wloads:
        load.start()
    meet((('dm', nd), ('tp', nt)))
    o_copies = {}
    for rel in (2, 1, 3) if nd == 4 else range(1, nd):
        to = lax.rem(dm + rel, nd)
        o_copies[rel] = remote(o_ref, o_all.at[dm], o_ss.at[rel], o_rs.at[rel], 'dm', to)
        o_copies[rel].start()
        sends.append(o_copies[rel])
    if wg.shape[0] > ff:
        for w in (wg, wu, wd):
            w[ff:, :] = jnp.zeros((w.shape[0] - ff, width), BF16)
    wloads[0].wait()
    for rel in range(nd):
        j = lax.rem(dm + nd - rel, nd)
        if rel:
            o_copies[rel].wait_recv()
            o = o_all[j]
        else:
            o = o_ref[...]
        part = jnp.dot(o, wo[...], preferred_element_type=F32)
        for c in range(per):
            t = j * per + c
            acc32[t] = part[c * rows_t:(c + 1) * rows_t]
            rs1_s[t] = part[c * rows_t:(c + 1) * rows_t].astype(BF16)
            far = lax.rem(t + nt - tp, nt)

            @pl.when(far != 0)
            def _(t=t, far=far):
                remote(rs1_s.at[t], rs1_r.at[tp], a_ss.at[far], a_rs.at[far], 'tp', t).start()

    def reduced(acc, recv, s_sems, r_sems, sent):
        total = acc[tp]
        for rel in range(1, nt):
            frm = lax.rem(tp + nt - rel, nt)
            copy = remote(sent.at[frm], recv.at[frm], s_sems.at[rel], r_sems.at[rel], 'tp', frm)
            copy.wait_recv()
            total = total + recv[frm].astype(F32)
            sends.append(copy)
        return total.astype(BF16)

    def gather(buf, s_sems, r_sems):
        out = {}
        for rel in range(1, nt):
            out[rel] = remote(buf.at[tp], buf.at[tp], s_sems.at[rel], r_sems.at[rel], 'tp', lax.rem(tp + rel, nt))
            out[rel].start()
            sends.append(out[rel])
        return out

    wloads[4].wait()
    wloads[5].wait()
    attn = reduced(acc32, rs1_r, a_ss, a_rs, rs1_s)
    hid = hid_ref[pl.ds(pl.multiple_of(tp * rows_t, rows_t), rows_t), :]
    mine = (hid.astype(F32) + attn.astype(F32)).astype(BF16)
    mid[tp] = mine
    mid_copies = gather(mid, b_ss, b_rs)
    y = mine.astype(F32)
    st_dm[dm] = column_to_row(jnp.sum(y * y, axis=1, keepdims=True), 128)
    sd_copies = []
    for rel in range(1, nd):
        copy = remote(st_dm.at[dm], st_dm.at[dm], sd_ss.at[rel], sd_rs.at[rel], 'dm', lax.rem(dm + rel, nd))
        copy.start()
        sd_copies.append(copy)
    sends.extend(sd_copies)
    for copy in sd_copies:
        copy.wait_recv()
    total = st_dm[0]
    for i in range(1, nd):
        total = total + st_dm[i]
    st_tp[tp] = total
    st_copies = gather(st_tp, st_ss, st_rs)
    gain = gain_ref[...].astype(F32).reshape(1, width)
    for rel in range(nt):
        t = lax.rem(tp + nt - rel, nt)
        if rel:
            st_copies[rel].wait_recv()
            mid_copies[rel].wait_recv()
        scale = lax.rsqrt(row_to_column(st_tp[t], rows_t) / width_full + EPS)
        x2[pl.ds(pl.multiple_of(t * rows_t, rows_t), rows_t), :] = (mid[t].astype(F32) * scale * gain).astype(BF16)
    wloads[1].wait()
    wloads[2].wait()
    half = fc // 2
    left, right, far = (lax.rem(dm + i, nd) for i in (nd - 1, 1, 2))

    def gate_up(to, h):
        at = pl.ds(pl.multiple_of(to * fc + h * half, 16), half)
        both = jnp.concatenate([wg[at, :], wu[at, :]], axis=0)
        return lax.dot_general(both, x2[...], NT_DIMS, preferred_element_type=F32)

    def send(src, dst, k, to):
        copy = remote(src, dst, g_ss.at[k], g_rs.at[k], 'dm', to)
        copy.start()
        sends.append(copy)
        return copy

    steps = ((right, 0), (left, 1))
    relays = []
    for to, h in steps:
        gu_far[h] = gate_up(far, h).astype(BF16)
        relays.append(send(gu_far.at[h], gu_relay.at[h], h, to))
    arrived = []
    for to, h in steps:
        gu_s[h, 1 - h] = gate_up(to, 1 - h).astype(BF16)
        arrived.append(send(gu_s.at[h, 1 - h], gu_r.at[h, 1 - h], 2 + h, to))
    for to, h in steps:
        gu_own[2 + h] = gate_up(to, h)
    for h in range(2):
        gu_own[h] = gate_up(dm, h)
    for to, h in steps:
        relays[h].wait_recv()
        gu_s[h, h] = (gu_own[2 + h] + gu_relay[h].astype(F32)).astype(BF16)
        arrived.append(send(gu_s.at[h, h], gu_r.at[h, h], 4 + h, to))
    for copy in arrived:
        copy.wait_recv()
    sums = [gu_own[h] + gu_r[0, h].astype(F32) + gu_r[1, h].astype(F32) for h in range(2)]
    gate = jnp.concatenate([x[:half] for x in sums], axis=0)
    up = jnp.concatenate([x[half:] for x in sums], axis=0)
    m_all[dm] = (gate / (1.0 + jnp.exp(-gate)) * up).astype(BF16)
    m_copies = {}
    for rel in (2, 1, 3) if nd == 4 else range(1, nd):
        m_copies[rel] = remote(m_all.at[dm], m_all.at[dm], m_ss.at[rel], m_rs.at[rel], 'dm', lax.rem(dm + rel, nd))
        m_copies[rel].start()
        sends.append(m_copies[rel])
    wloads[3].wait()
    for k, rel in enumerate((0, 1, 3, 2) if nd == 4 else range(nd)):
        j = lax.rem(dm + nd - rel, nd)
        if rel:
            m_copies[rel].wait_recv()
        part = lax.dot_general(m_all[j], wd[pl.ds(pl.multiple_of(j * fc, 16), fc), :], TN_DIMS, preferred_element_type=F32)
        for t in range(nt):
            piece = part[t * rows_t:(t + 1) * rows_t]
            acc32[t] = piece if k == 0 else acc32[t] + piece
    for t in range(nt):
        rs2_s[t] = acc32[t].astype(BF16)
    for rel in range(1, nt):
        to = lax.rem(tp + rel, nt)
        remote(rs2_s.at[to], rs2_r.at[tp], c_ss.at[rel], c_rs.at[rel], 'tp', to).start()
    mlp = reduced(acc32, rs2_r, c_ss, c_rs, rs2_s)
    fin[tp] = (mid[tp].astype(F32) + mlp.astype(F32)).astype(BF16)
    f_copies = gather(fin, d_ss, d_rs)
    for rel in range(nt):
        t = lax.rem(tp + nt - rel, nt)
        if rel:
            f_copies[rel].wait_recv()
        out_ref[pl.ds(pl.multiple_of(t * rows_t, rows_t), rows_t), :] = fin[t]
    for copy in sends:
        copy.wait_send()


VMEM = pl.BlockSpec(memory_space=pltpu.VMEM)
SEM = pl.BlockSpec(memory_space=pltpu.SEMAPHORE)
SMEM = pl.BlockSpec(memory_space=pltpu.SMEM)
HBM = pl.BlockSpec(memory_space=pltpu.HBM)
MIB = 1 << 20


def solution(mesh):
    nd = mesh.shape['dm']
    nt = mesh.shape['tp']
    row_spec = P('dp', 'dm')
    cache_spec = P(('dp', 'dm'), None, 'tp', None)
    batch_spec = P(('dp', 'dm'))
    rope_spec = P(('dp', 'dm'), None)
    in_specs = (row_spec, P('dm', 'tp', None), P('dm', 'tp', None), P('dm', 'tp', None), P('tp', None, 'dm'), P('dm', 'tp'), P('dm', 'tp'), P('tp', 'dm'), P('dm'), P('dm'), cache_spec, cache_spec, batch_spec, rope_spec, rope_spec)
    out_specs = (row_spec, cache_spec, cache_spec)
    dma = pltpu.SemaphoreType.DMA

    def local_layer(hidden, w_q, w_k, w_v, w_o, w_gate, w_up, w_down, norm_attn, norm_mlp, k_cache, v_cache, seq_lens, rope_cos, rope_sin):
        batch, width = hidden.shape
        width_full = width * nd
        _, heads, dim = w_q.shape
        rows, seq = k_cache.shape[:2]
        cols = heads * dim
        ff = w_gate.shape[1]
        def hbm(x):
            return pltpu.with_memory_space_constraint(x, pltpu.HBM)

        def vmem(x):
            return pltpu.with_memory_space_constraint(x, pltpu.VMEM)

        flat = (rows, seq * heads, dim)
        groups = rows // 8
        q, k, v = pl.pallas_call(
            functools.partial(qkv_kernel, nd, heads, width_full),
            out_shape=(jax.ShapeDtypeStruct((rows // 8, heads, 8, dim), F32),
                       jax.ShapeDtypeStruct((heads, rows, dim), F32),
                       jax.ShapeDtypeStruct((heads, rows, dim), F32)),
            in_specs=[HBM] * 7,
            out_specs=(VMEM, VMEM, VMEM),
            scratch_shapes=[
                pltpu.VMEM((batch, width), BF16),
                pltpu.VMEM((width,), BF16),
                pltpu.VMEM(rope_cos.shape, F32),
                pltpu.VMEM(rope_sin.shape, F32),
                pltpu.VMEM((3, width * heads, dim), BF16),
                pltpu.VMEM((width // 8 * heads, dim), F32),
                pltpu.VMEM((3, width, cols), BF16),
                pltpu.VMEM((nd, 1, batch), F32),
                pltpu.VMEM((3, nd, rows, cols), F32),
                pltpu.VMEM((3, nd, rows, cols), BF16),
                pltpu.VMEM((3, nd, rows, cols), BF16),
                dma((4,)), dma((3,)), dma((nd,)), dma((nd,)), dma((3, nd)), dma((3, nd)),
            ],
            compiler_params=pltpu.CompilerParams(collective_id=0, has_side_effects=True, vmem_limit_bytes=16 * MIB),
            cost_estimate=pl.CostEstimate(flops=10_000_000_000, bytes_accessed=32 * MIB, transcendentals=0),
            name='qkv',
        )(hbm(hidden), hbm(norm_attn), hbm(w_q.reshape(width * heads, dim)), hbm(w_k.reshape(width * heads, dim)),
          hbm(w_v.reshape(width * heads, dim)), hbm(rope_cos), hbm(rope_sin))

        o, k_new, v_new = pl.pallas_call(
            attend_kernel,
            out_shape=(jax.ShapeDtypeStruct((rows, cols), BF16), jax.ShapeDtypeStruct(flat, BF16), jax.ShapeDtypeStruct(flat, BF16)),
            in_specs=[SMEM, VMEM, VMEM, VMEM, VMEM, VMEM],
            out_specs=(VMEM, HBM, HBM),
            scratch_shapes=[
                pltpu.VMEM((2, rows * 16, dim), F32),
                pltpu.VMEM((2, rows, 16, dim), BF16),
                pltpu.VMEM((rows, cols), F32),
                dma((2, rows // 8)), dma((2, rows)),
            ],
            compiler_params=pltpu.CompilerParams(vmem_limit_bytes=8 * MIB),
            name='attend',
        )(seq_lens, q, k, v, vmem(k_cache.reshape(flat)), vmem(v_cache.reshape(flat)))

        fc = -(-ff // (nd * 32)) * 32
        rows_t = batch // nt
        slab = (nt, rows_t, width)
        out = pl.pallas_call(
            functools.partial(mlp_kernel, nd, nt, fc, width_full),
            out_shape=jax.ShapeDtypeStruct((batch, width), BF16),
            in_specs=[VMEM] + [HBM] * 6,
            out_specs=VMEM,
            scratch_shapes=[
                pltpu.VMEM((batch, width), BF16),
                pltpu.VMEM((width,), BF16),
                pltpu.VMEM((cols, width), BF16),
                pltpu.VMEM((nd * fc, width), BF16),
                pltpu.VMEM((nd * fc, width), BF16),
                pltpu.VMEM((nd * fc, width), BF16),
                pltpu.VMEM((nd, rows, cols), BF16),
                pltpu.VMEM(slab, F32),
                pltpu.VMEM(slab, BF16),
                pltpu.VMEM(slab, BF16),
                pltpu.VMEM(slab, BF16),
                pltpu.VMEM((nd, 1, 128), F32),
                pltpu.VMEM((nt, 1, 128), F32),
                pltpu.VMEM((batch, width), BF16),
                pltpu.VMEM((2, fc, batch), BF16),
                pltpu.VMEM((2, fc, batch), BF16),
                pltpu.VMEM((2, 2, fc, batch), BF16),
                pltpu.VMEM((2, 2, fc, batch), BF16),
                pltpu.VMEM((4, fc, batch), F32),
                pltpu.VMEM((nd, fc, batch), BF16),
                pltpu.VMEM(slab, BF16),
                pltpu.VMEM(slab, BF16),
                pltpu.VMEM(slab, BF16),
                dma((6,)), dma((nd,)), dma((nd,)), dma((nt,)), dma((nt,)), dma((nt,)), dma((nt,)),
                dma((nd,)), dma((nd,)), dma((nt,)), dma((nt,)), dma((6,)), dma((6,)), dma((nd,)), dma((nd,)),
                dma((nt,)), dma((nt,)), dma((nt,)), dma((nt,)),
            ],
            compiler_params=pltpu.CompilerParams(collective_id=1, has_side_effects=True, vmem_limit_bytes=24 * MIB),
            name='mlp',
        )(o, hbm(hidden), hbm(norm_mlp), hbm(w_o.reshape(cols, width)), hbm(w_gate.T), hbm(w_up.T), hbm(w_down))
        return out, k_new.reshape(k_cache.shape), v_new.reshape(v_cache.shape)

    return jax.shard_map(local_layer, mesh=mesh, in_specs=in_specs, out_specs=out_specs, check_vma=False)
```
